128 devices in a mesh: bank: 8 (over x, core), lane: 16 (over z, y).
Axes of the slice: x: 4, y: 4, z: 4, core: 2. Of those that a mesh axis runs over, the one named last changes fastest.
Arguments:
- amplitudes: float32 [2, 2048, 128, 128], P(None, ('bank', 'lane')), may hold values from -6 to 6
- energies: float32 [2048, 128, 128], P(('bank', 'lane')), may hold values from -2 to 2
- diagonal_angles: float32 [2, 128], replicated, may hold values from 0.3 to 1.2
- turn_angles: float32 [2, 4], replicated, may hold values from 0.3 to 1.2
Outputs:
- state_after: float32 [2, 2048, 128, 128], P(None, ('bank', 'lane'))
The draws below stay inside these ranges and needn't reach their ends.
All inputs are finite; a program needn't handle non-finite values.
Results may differ from the reference program's by a relative error of at most 0.0003.
Values sent between devices are 32-bit elements; how exact they have to be, the bound alone decides.
A program may use at most 64 MiB of HBM per device.

```python
import jax
import jax.numpy as jnp
from jax import lax

BLOCKS_DEV = 16
ROWS = 128
LANES = 128
BLOCKS = 2048
LAYERS = 2
N_BANK = 8
N_LANE = 16


def shard_levels(key, dims, cuts, smallest, high):
    def one(axis_at, blocks):
        heights = jax.random.uniform(jax.random.fold_in(jax.random.fold_in(key, 6), axis_at), (blocks,), jnp.float32, smallest / len(cuts), high / len(cuts))
        return jnp.repeat(jnp.exp(heights), dims[axis_at] // blocks).reshape((-1,) + (1,) * (len(dims) - axis_at - 1))

    loudness = one(*cuts[0])
    for cut in cuts[1:]:
        loudness = loudness * one(*cut)
    return loudness


def gaussian(own_key, extent, width, most, cuts=(), held_as=jnp.bfloat16):
    drawn = width * jax.random.normal(own_key, extent, jnp.float32)
    if cuts:
        drawn = drawn * shard_levels(own_key, extent, cuts, -0.22, 0.18)
    return jnp.clip(drawn, -most, most).astype(held_as)


def setup_inputs(seed: int = 0) -> dict:
    splits = jax.random.split(jax.random.key(seed), 5)
    amplitudes = gaussian(splits[0], (2, BLOCKS, ROWS, LANES), 1.0, 6.0, ((1, 128),), jnp.float32)
    energies = jnp.clip(jax.random.uniform(splits[1], (BLOCKS, ROWS, LANES), jnp.float32, -2.0, 2.0) * shard_levels(splits[1], (BLOCKS, ROWS, LANES), ((0, 128),), -0.4, 0.0), -2.0, 2.0)
    diagonal_angles = jnp.clip(jax.random.uniform(splits[2], (LAYERS, LANES), jnp.float32, 0.3, 1.2), 0.3, 1.2)
    turn_angles = jnp.clip(jax.random.uniform(splits[3], (LAYERS, 4), jnp.float32, 0.3, 1.2), 0.3, 1.2)
    return {"amplitudes": amplitudes, "energies": energies, "diagonal_angles": diagonal_angles, "turn_angles": turn_angles}


def count_bits(values, count):
    places = jnp.arange(count.bit_length() - 1, dtype=jnp.int32)
    return jnp.sum((values[..., None] >> places) & 1, axis=-1)


def plane_table(count, angle):
    rank = jnp.arange(count, dtype=jnp.int32)
    apart = count_bits(rank[:, None] ^ rank[None, :], count)
    minus = count_bits(rank[:, None] & (rank[:, None] ^ rank[None, :]), count)
    bits = count.bit_length() - 1
    size = jnp.cos(angle) ** (bits - apart).astype(jnp.float32) * jnp.sin(angle) ** apart.astype(jnp.float32)
    return size * jnp.where(minus % 2 == 1, -1.0, 1.0).astype(jnp.float32)


def mix_dim(values, dim, angle):
    real_part = plane_table(values.shape[dim], angle)
    def times(table):
        moved = jnp.tensordot(values, table, axes=([dim], [0]), precision=lax.Precision.HIGHEST)
        return jnp.moveaxis(moved, -1, dim)
    return times(real_part)


def phase_step(values, levels, angle):
    turn = angle * levels
    return jnp.stack([values[0] * jnp.cos(turn) + values[1] * jnp.sin(turn), values[1] * jnp.cos(turn) - values[0] * jnp.sin(turn)])


def reference(amplitudes, energies, diagonal_angles, turn_angles):
    values = amplitudes
    for layer in range(LAYERS):
        values = phase_step(values, energies, diagonal_angles[layer])
        values = mix_dim(values, 3, turn_angles[layer, 0])
        values = mix_dim(values, 2, turn_angles[layer, 1])
        parts = values.reshape(2, N_BANK, N_LANE, BLOCKS_DEV, ROWS, LANES)
        parts = mix_dim(parts, 1, turn_angles[layer, 2])
        parts = mix_dim(parts, 2, turn_angles[layer, 3])
        parts = mix_dim(parts, 3, turn_angles[layer, 2])
        values = parts.reshape(values.shape)
    return values
```

```python
import functools

import jax
import jax.numpy as jnp
from jax import lax
from jax.experimental import pallas as pl
from jax.experimental.pallas import tpu as pltpu
from jax.sharding import PartitionSpec as P

N_DEV = 128
N_LANE = 16
BITS = 7


def place():
    return lax.axis_index("bank"), lax.axis_index("lane")


def partner(step):
    bank, lane = place()
    step = lax.rem(step * 37, N_DEV)
    x = lax.rem(bank // 2 + step // 32, 4)
    core = lax.rem(lax.rem(bank, 2) + lax.rem(step // 16, 2), 2)
    z = lax.rem(lane // 4 + lax.rem(step // 4, 4), 4)
    y = lax.rem(lax.rem(lane, 4) + lax.rem(step, 4), 4)
    to_bank = x * 2 + core
    to_lane = z * 4 + y
    return (to_bank, to_lane), to_bank * N_LANE + to_lane


def send_all(pick_src, pick_dst, send_sem, recv_sem):
    bank, lane = place()
    me = bank * N_LANE + lane

    def one(step, carry):
        device, index = partner(step)
        pltpu.make_async_remote_copy(
            src_ref=pick_src(index),
            dst_ref=pick_dst(me),
            send_sem=send_sem,
            recv_sem=recv_sem,
            device_id=device,
            device_id_type=pl.DeviceIdType.MESH,
        ).start()
        return carry

    lax.fori_loop(1, N_DEV, one, 0)


def wait_bytes(ref, sem):
    pltpu.make_async_copy(ref, ref, sem).wait()


def cos_sin(half):
    sq = half * half
    s = 1.0 / 6227020800.0
    for term in (-1.0 / 39916800.0, 1.0 / 362880.0, -1.0 / 5040.0, 1.0 / 120.0, -1.0 / 6.0):
        s = s * sq + term
    s = half + half * (sq * s)
    c = 1.0 / 479001600.0
    for term in (-1.0 / 3628800.0, 1.0 / 40320.0, -1.0 / 720.0, 1.0 / 24.0, -0.5):
        c = c * sq + term
    c = 1.0 + sq * c
    twice = s + s
    return 1.0 - twice * s, twice * c


def butterfly(tiles, tan):
    tiles = list(tiles)
    step = 1
    while step < len(tiles):
        for i in range(len(tiles)):
            if i & step:
                continue
            u, v = tiles[i], tiles[i + step]
            tiles[i] = u - tan * v
            tiles[i + step] = v + tan * u
        step *= 2
    return tiles


def rotate_phase(re, im, half):
    c, s = cos_sin(half)
    return re * c + im * s, im * c - re * s


def sublane_mix(values, tan):
    place_in = lax.broadcasted_iota(jnp.int32, values.shape, 1)
    for step in (4, 2, 1):
        upper = (place_in // step) % 2 == 1
        below = pltpu.roll(values, step, 1)
        other = below if step == 4 else jnp.where(upper, below, pltpu.roll(values, 8 - step, 1))
        values = values + jnp.where(upper, tan, -tan) * other
    return values


def lane_table(cos, sin, scale):
    row = lax.broadcasted_iota(jnp.int32, (128, 128), 0)
    col = lax.broadcasted_iota(jnp.int32, (128, 128), 1)
    table = jnp.broadcast_to(scale, (128, 128))
    for bit in range(BITS):
        r = (row // 2**bit) % 2
        c = (col // 2**bit) % 2
        table = table * jnp.where(r == c, cos, jnp.where(r > c, -sin, sin))
    high = table.astype(jnp.bfloat16)
    low = (table - high.astype(jnp.float32)).astype(jnp.bfloat16)
    both = jnp.concatenate([high, low], axis=1)
    return jnp.concatenate([both, both], axis=0)


def lane_mix(values, table):
    high = values.astype(jnp.bfloat16)
    low = (values - high.astype(jnp.float32)).astype(jnp.bfloat16)
    parts = jnp.concatenate([high, low], axis=1)
    out = jnp.dot(parts, table, preferred_element_type=jnp.float32)
    return out[:, :128] + out[:, 128:]


def kernel(amp, energy, diag, turn, out, a_in, e_in, e_rx, fwd, mid, back, fin, tables, tans, sems, sends, recvs):
    bank, lane = place()
    me = bank * N_LANE + lane

    get_e = pltpu.make_async_copy(energy, e_in, sems.at[0])
    get_a = pltpu.make_async_copy(amp, a_in, sems.at[1])
    get_e.start()
    get_a.start()

    cos, sin = cos_sin(turn[...] * 0.5)
    tan = sin / cos
    for layer in range(2):
        for group in range(4):
            tans[layer, group] = jnp.broadcast_to(tan[layer : layer + 1, group : group + 1], (8, 128))
        c = [cos[layer : layer + 1, g : g + 1] for g in range(4)]
        c12 = c[1] * c[2]
        c12_2 = c12 * c12
        c3_2 = c[3] * c[3]
        scale = c12_2 * c12_2 * c12_2 * c12 * c3_2 * c3_2
        tables[layer] = lane_table(c[0], sin[layer : layer + 1, 0:1], scale)

    get_e.wait()
    send_all(lambda i: e_in.at[i], lambda i: e_rx.at[i], sends.at[0], recvs.at[0])
    get_a.wait()
    e_rx[me] = e_in[me]

    def first(i, carry):
        at = pl.ds(i * 8, 8)
        half = e_in[at] * (diag[0:1, :] * 0.5).reshape(1, 1, 1, 128)
        re, im = rotate_phase(a_in[0, at], a_in[1, at], half)
        values = jnp.concatenate([re, im], axis=0)
        mixed = lane_mix(values.reshape(256, 128), tables[0]).reshape(32, 8, 128)
        mixed = sublane_mix(mixed, tans[0, 1, 0:1, :].reshape(1, 1, 128))
        mixed = mixed.reshape(2, 16, 8, 128)
        tan1 = tans[0, 1]
        for part in range(2):
            tiles = butterfly([mixed[part, j] for j in range(16)], tan1)
            for j in range(16):
                a_in[part, i * 8 + j // 2, j % 2] = tiles[j]
        return carry

    lax.fori_loop(0, 16, first, 0)

    tan2 = tans[0, 2]
    for k in range(2):

        def blocks(i, carry):
            part, row = i // 8, lax.rem(i, 8)
            tiles = butterfly([a_in[part, b * 8 + row, k] for b in range(16)], tan2)
            for b in range(16):
                fwd[k, b * 8 + row, part] = tiles[b]
            return carry

        lax.fori_loop(0, 16, blocks, 0)
        send_all(
            lambda i: fwd.at[k, i], lambda i: mid.at[k, i], sends.at[1 + k], recvs.at[1 + k]
        )
        mid[k, me] = fwd[k, me]

    wait_bytes(e_rx.at[pl.ds(0, N_DEV - 1)], recvs.at[0])
    for k in range(2):
        wait_bytes(mid.at[k, pl.ds(0, N_DEV - 1)], recvs.at[1 + k])

        def lanes_1(i, carry):
            b, part = i // 2, lax.rem(i, 2)
            tiles = butterfly([mid[k, b * 16 + l, part] for l in range(16)], tans[0, 3])
            for l in range(16):
                mid[k, b * 16 + l, part] = tiles[l]
            return carry

        lax.fori_loop(0, 16, lanes_1, 0)

        def banks(l, carry):
            re = butterfly([mid[k, b * 16 + l, 0] for b in range(8)], tans[0, 2])
            im = butterfly([mid[k, b * 16 + l, 1] for b in range(8)], tans[0, 2])
            angle = diag[1:2, :] * 0.5
            for b in range(8):
                re[b], im[b] = rotate_phase(re[b], im[b], e_rx[b * 16 + l, k] * angle)
            re = butterfly(re, tans[1, 2])
            im = butterfly(im, tans[1, 2])
            for b in range(8):
                mid[k, b * 16 + l, 0] = re[b]
                mid[k, b * 16 + l, 1] = im[b]
            return carry

        lax.fori_loop(0, 16, banks, 0)

        def lanes_2(b, carry):
            both = []
            for part in range(2):
                tiles = butterfly([mid[k, b * 16 + l, part] for l in range(16)], tans[1, 3])
                both.append(jnp.stack(tiles))
            values = jnp.stack(both).reshape(256, 128)
            mixed = lane_mix(values, tables[1]).reshape(32, 8, 128)
            mixed = sublane_mix(mixed, tans[1, 1, 0:1, :].reshape(1, 1, 128))
            mixed = mixed.reshape(2, 16, 8, 128)
            for part in range(2):
                back[k, part, pl.ds(b * 16, 16)] = mixed[part]
            return carry

        lax.fori_loop(0, 8, lanes_2, 0)
        for part in range(2):
            n = 3 + 2 * k + part
            send_all(
                lambda i: back.at[k, part, i], lambda i: fin.at[k, part, i], sends.at[n], recvs.at[n]
            )
            fin[k, part, me] = back[k, part, me]

    for k in range(2):
        for part in range(2):
            n = 3 + 2 * k + part
            wait_bytes(fin.at[k, part, pl.ds(0, N_DEV - 1)], recvs.at[n])

            def rows(b, carry):
                tiles = butterfly([fin[k, part, b * 8 + r] for r in range(8)], tans[1, 1])
                for r in range(8):
                    fin[k, part, b * 8 + r] = tiles[r]
                return carry

            lax.fori_loop(0, 16, rows, 0)

            def last(r, carry):
                tiles = butterfly([fin[k, part, b * 8 + r] for b in range(16)], tans[1, 2])
                if k == 0:
                    for b in range(16):
                        fin[0, part, b * 8 + r] = tiles[b]
                else:
                    t = tans[1, 1]
                    for b in range(16):
                        u = fin[0, part, b * 8 + r]
                        v = tiles[b]
                        a_in[part, b * 8 + r, 0] = u - t * v
                        a_in[part, b * 8 + r, 1] = v + t * u
                return carry

            lax.fori_loop(0, 8, last, 0)
            if k == 1:
                pltpu.make_async_copy(a_in.at[part], out.at[part], sems.at[part]).start()
    for part in range(2):
        pltpu.make_async_copy(a_in.at[part], out.at[part], sems.at[part]).wait()

    wait_bytes(e_in.at[pl.ds(0, N_DEV - 1)], sends.at[0])
    for k in range(2):
        wait_bytes(fwd.at[k, pl.ds(0, N_DEV - 1)], sends.at[1 + k])
        for part in range(2):
            wait_bytes(back.at[k, part, pl.ds(0, N_DEV - 1)], sends.at[3 + 2 * k + part])


def body(amplitudes, energies, diagonal_angles, turn_angles):
    f32 = jnp.float32
    anywhere = pl.BlockSpec(memory_space=pl.ANY)
    vmem = pl.BlockSpec(memory_space=pltpu.VMEM)
    out = pl.pallas_call(
        kernel,
        out_shape=jax.ShapeDtypeStruct((2, N_DEV, 2, 8, 128), f32),
        in_specs=[anywhere, anywhere, vmem, vmem],
        out_specs=anywhere,
        scratch_shapes=[
            pltpu.VMEM((2, N_DEV, 2, 8, 128), f32),
            pltpu.VMEM((N_DEV, 2, 8, 128), f32),
            pltpu.VMEM((N_DEV, 2, 8, 128), f32),
            pltpu.VMEM((2, N_DEV, 2, 8, 128), f32),
            pltpu.VMEM((2, N_DEV, 2, 8, 128), f32),
            pltpu.VMEM((2, 2, N_DEV, 8, 128), f32),
            pltpu.VMEM((2, 2, N_DEV, 8, 128), f32),
            pltpu.VMEM((2, 256, 256), jnp.bfloat16),
            pltpu.VMEM((2, 4, 8, 128), f32),
            pltpu.SemaphoreType.DMA((2,)),
            pltpu.SemaphoreType.DMA((7,)),
            pltpu.SemaphoreType.DMA((7,)),
        ],
        compiler_params=pltpu.CompilerParams(has_side_effects=True),
        name="register",
    )(
        amplitudes.reshape(2, N_DEV, 2, 8, 128),
        energies.reshape(N_DEV, 2, 8, 128),
        diagonal_angles,
        turn_angles,
    )
    return out.reshape(2, 16, 128, 128)


def solution(mesh):
    split = P(None, ("bank", "lane"), None, None)
    in_specs = (split, P(("bank", "lane"), None, None), P(), P())
    return jax.shard_map(body, mesh=mesh, in_specs=in_specs, out_specs=split, check_vma=False)
```

```python
import itertools

import jax
import jax.numpy as jnp
from jax import lax
from jax.experimental import pallas as pl
from jax.experimental.pallas import tpu as pltpu
from jax.sharding import PartitionSpec as P

N_DEV = 128
N_LANE = 16
BITS = 7


def place():
    return lax.axis_index("bank"), lax.axis_index("lane")


def hops(step):
    return min(step, 4 - step)


STEPS = sorted(
    (s for s in itertools.product(range(4), range(2), range(4), range(4)) if any(s)),
    key=lambda s: -hops(s[0]) - hops(s[2]) - hops(s[3]),
)


def others():
    bank, lane = place()
    x, core, z, y = bank // 2, lax.rem(bank, 2), lane // 4, lax.rem(lane, 4)
    xs = [lax.rem(x + s, 4) * 2 for s in range(4)]
    cores = [core, 1 - core]
    zs = [lax.rem(z + s, 4) * 4 for s in range(4)]
    ys = [lax.rem(y + s, 4) for s in range(4)]
    banks = {(i, j): xs[i] + cores[j] for i in range(4) for j in range(2)}
    lanes = {(i, j): zs[i] + ys[j] for i in range(4) for j in range(4)}
    found = []
    for sx, sc, sz, sy in STEPS:
        to_bank, to_lane = banks[sx, sc], lanes[sz, sy]
        found.append(((to_bank, to_lane), to_bank * N_LANE + to_lane))
    return found


def send_all(devices, pick_src, dst, send_sem, recv_sem):
    for device, index in devices:
        pltpu.make_async_remote_copy(
            src_ref=pick_src(index),
            dst_ref=dst,
            send_sem=send_sem,
            recv_sem=recv_sem,
            device_id=device,
            device_id_type=pl.DeviceIdType.MESH,
        ).start()


def wait_bytes(ref, sem):
    pltpu.make_async_copy(ref, ref, sem).wait()


def cos_sin(half):
    sq = half * half
    s = 1.0 / 6227020800.0
    for term in (-1.0 / 39916800.0, 1.0 / 362880.0, -1.0 / 5040.0, 1.0 / 120.0, -1.0 / 6.0):
        s = s * sq + term
    s = half + half * (sq * s)
    c = 1.0 / 479001600.0
    for term in (-1.0 / 3628800.0, 1.0 / 40320.0, -1.0 / 720.0, 1.0 / 24.0, -0.5):
        c = c * sq + term
    c = 1.0 + sq * c
    twice = s + s
    return 1.0 - twice * s, twice * c


def butterfly(tiles, tan):
    tiles = list(tiles)
    step = 1
    while step < len(tiles):
        for i in range(len(tiles)):
            if i & step:
                continue
            u, v = tiles[i], tiles[i + step]
            tiles[i] = u - tan * v
            tiles[i + step] = v + tan * u
        step *= 2
    return tiles


def rotate_phase(re, im, half):
    c, s = cos_sin(half)
    return re * c + im * s, im * c - re * s


def sublane_mix(values, tan):
    place_in = lax.broadcasted_iota(jnp.int32, values.shape, 1)
    for step in (4, 2, 1):
        upper = (place_in // step) % 2 == 1
        below = pltpu.roll(values, step, 1)
        other = below if step == 4 else jnp.where(upper, below, pltpu.roll(values, 8 - step, 1))
        values = values + jnp.where(upper, tan, -tan) * other
    return values


def lane_table(cos, sin, scale):
    row = lax.broadcasted_iota(jnp.int32, (128, 128), 0)
    col = lax.broadcasted_iota(jnp.int32, (128, 128), 1)
    table = jnp.broadcast_to(scale, (128, 128))
    for bit in range(BITS):
        r = (row // 2**bit) % 2
        c = (col // 2**bit) % 2
        table = table * jnp.where(r == c, cos, jnp.where(r > c, -sin, sin))
    high = table.astype(jnp.bfloat16)
    low = (table - high.astype(jnp.float32)).astype(jnp.bfloat16)
    both = jnp.concatenate([high, low], axis=1)
    return jnp.concatenate([both, both], axis=0)


def lane_mix(values, table):
    high = values.astype(jnp.bfloat16)
    low = (values - high.astype(jnp.float32)).astype(jnp.bfloat16)
    parts = jnp.concatenate([high, low], axis=1)
    out = jnp.dot(parts, table, preferred_element_type=jnp.float32)
    return out[:, :128] + out[:, 128:]


def kernel(amp, energy, diag_any, turn_any, out, diag, turn, a_in, fwd, mid, back, fin, tables, tans, sems, sends, recvs):
    bank, lane = place()
    me = bank * N_LANE + lane
    scope = jax.named_scope

    gets = [pltpu.make_async_copy(energy.at[:, k], fwd.at[k, :, 2], sems.at[k]) for k in range(2)]
    gets += [pltpu.make_async_copy(amp, a_in, sems.at[2])]
    small = [pltpu.make_async_copy(diag_any, diag, sems.at[3]), pltpu.make_async_copy(turn_any, turn, sems.at[4])]
    for get in small + gets:
        get.start()

    devices = others()
    barrier = pltpu.get_barrier_semaphore()
    with scope("signals"):
        for device, _ in devices:
            pl.semaphore_signal(barrier, 1, device_id=device, device_id_type=pl.DeviceIdType.MESH)

    with scope("tables"):
        for get in small:
            get.wait()
        cos, sin = cos_sin(turn[...] * 0.5)
        tan = sin / cos
        for layer in range(2):
            for group in range(4):
                tans[layer, group] = jnp.broadcast_to(tan[layer : layer + 1, group : group + 1], (8, 128))
            c = [cos[layer : layer + 1, g : g + 1] for g in range(4)]
            c12 = c[1] * c[2]
            c12_2 = c12 * c12
            c3_2 = c[3] * c[3]
            scale = c12_2 * c12_2 * c12_2 * c12 * c3_2 * c3_2
            tables[layer] = lane_table(c[0], sin[layer : layer + 1, 0:1], scale)

    with scope("wait_in"):
        for get in gets:
            get.wait()

    def first(i, carry):
        at = pl.ds(i * 8, 8)
        angle = (diag[0:1, :] * 0.5).reshape(1, 1, 1, 128)
        half = jnp.stack([fwd[0, at, 2], fwd[1, at, 2]], axis=1) * angle
        re, im = rotate_phase(a_in[0, at], a_in[1, at], half)
        values = jnp.concatenate([re, im], axis=0)
        mixed = lane_mix(values.reshape(256, 128), tables[0]).reshape(32, 8, 128)
        mixed = sublane_mix(mixed, tans[0, 1, 0:1, :].reshape(1, 1, 128))
        mixed = mixed.reshape(2, 16, 8, 128)
        tan1 = tans[0, 1]
        for part in range(2):
            tiles = butterfly([mixed[part, j] for j in range(16)], tan1)
            for j in range(16):
                a_in[part, i * 8 + j // 2, j % 2] = tiles[j]
        return carry

    with scope("first"):
        lax.fori_loop(0, 16, first, 0)

    tan2 = tans[0, 2]
    for k in range(2):

        def blocks(i, carry):
            part, row = i // 8, lax.rem(i, 8)
            tiles = butterfly([a_in[part, b * 8 + row, k] for b in range(16)], tan2)
            for b in range(16):
                fwd[k, b * 8 + row, part] = tiles[b]
            return carry

        with scope(f"blocks_{k}"):
            lax.fori_loop(0, 16, blocks, 0)
        if k == 0:
            with scope("barrier"):
                pl.semaphore_wait(barrier, N_DEV - 1)
        with scope(f"send_f{k}"):
            send_all(devices, lambda i: fwd.at[k, i], mid.at[k, me], sends.at[k], recvs.at[k])
        mid[k, me] = fwd[k, me]

    for k in range(2):
        with scope(f"wait_m{k}"):
            wait_bytes(mid.at[k, pl.ds(0, N_DEV - 1)], recvs.at[k])

        def lanes_1(i, carry):
            b, part = i // 2, lax.rem(i, 2)
            tiles = butterfly([mid[k, b * 16 + l, part] for l in range(16)], tans[0, 3])
            for l in range(16):
                mid[k, b * 16 + l, part] = tiles[l]
            return carry

        def banks(l, carry):
            re = butterfly([mid[k, b * 16 + l, 0] for b in range(8)], tans[0, 2])
            im = butterfly([mid[k, b * 16 + l, 1] for b in range(8)], tans[0, 2])
            angle = diag[1:2, :] * 0.5
            for b in range(8):
                re[b], im[b] = rotate_phase(re[b], im[b], mid[k, b * 16 + l, 2] * angle)
            re = butterfly(re, tans[1, 2])
            im = butterfly(im, tans[1, 2])
            for b in range(8):
                mid[k, b * 16 + l, 0] = re[b]
                mid[k, b * 16 + l, 1] = im[b]
            return carry

        def lanes_2(b, carry):
            both = []
            for part in range(2):
                tiles = butterfly([mid[k, b * 16 + l, part] for l in range(16)], tans[1, 3])
                both.append(jnp.stack(tiles))
            values = jnp.stack(both).reshape(256, 128)
            mixed = lane_mix(values, tables[1]).reshape(32, 8, 128)
            mixed = sublane_mix(mixed, tans[1, 1, 0:1, :].reshape(1, 1, 128))
            mixed = mixed.reshape(2, 16, 8, 128)
            for part in range(2):
                back[k, pl.ds(b * 16, 16), part] = mixed[part]
            return carry

        with scope(f"mid_{k}"):
            lax.fori_loop(0, 16, lanes_1, 0)
            lax.fori_loop(0, 16, banks, 0)
            lax.fori_loop(0, 8, lanes_2, 0)
        with scope(f"send_b{k}"):
            if k == 0:
                send_all(devices, lambda i: back.at[0, i], fin.at[0, me], sends.at[2], recvs.at[2])
            else:
                for part in range(2):
                    n = 3 + part
                    send_all(
                        devices, lambda i: back.at[1, i, part], fin.at[1, me, part], sends.at[n], recvs.at[n]
                    )
        fin[k, me] = back[k, me]

    for k in range(2):
        for part in range(2):
            with scope(f"wait_b{k}{part}"):
                if k == 1:
                    wait_bytes(fin.at[1, pl.ds(0, N_DEV - 1), part], recvs.at[3 + part])
                elif part == 0:
                    wait_bytes(fin.at[0, pl.ds(0, N_DEV - 1)], recvs.at[2])

            def rows(b, carry):
                tiles = butterfly([fin[k, b * 8 + r, part] for r in range(8)], tans[1, 1])
                for r in range(8):
                    fin[k, b * 8 + r, part] = tiles[r]
                return carry

            def last(r, carry):
                tiles = butterfly([fin[k, b * 8 + r, part] for b in range(16)], tans[1, 2])
                if k == 0:
                    for b in range(16):
                        fin[0, b * 8 + r, part] = tiles[b]
                else:
                    t = tans[1, 1]
                    for b in range(16):
                        u = fin[0, b * 8 + r, part]
                        v = tiles[b]
                        out[part, b * 8 + r, 0] = u - t * v
                        out[part, b * 8 + r, 1] = v + t * u
                return carry

            with scope(f"last_{k}{part}"):
                lax.fori_loop(0, 16, rows, 0)
                lax.fori_loop(0, 8, last, 0)

    for k in range(2):
        wait_bytes(fwd.at[k, pl.ds(0, N_DEV - 1)], sends.at[k])
    wait_bytes(back.at[0, pl.ds(0, N_DEV - 1)], sends.at[2])
    for part in range(2):
        wait_bytes(back.at[1, pl.ds(0, N_DEV - 1), part], sends.at[3 + part])


def body(amplitudes, energies, diagonal_angles, turn_angles):
    f32 = jnp.float32
    anywhere = pl.BlockSpec(memory_space=pl.ANY)
    vmem = pl.BlockSpec(memory_space=pltpu.VMEM)
    out = pl.pallas_call(
        kernel,
        out_shape=pltpu.VMEM((2, N_DEV, 2, 8, 128), f32),
        in_specs=[anywhere] * 4,
        out_specs=vmem,
        scratch_shapes=[
            pltpu.VMEM((2, 128), f32),
            pltpu.VMEM((2, 4), f32),
            pltpu.VMEM((2, N_DEV, 2, 8, 128), f32),
            pltpu.VMEM((2, N_DEV, 3, 8, 128), f32),
            pltpu.VMEM((2, N_DEV, 3, 8, 128), f32),
            pltpu.VMEM((2, N_DEV, 2, 8, 128), f32),
            pltpu.VMEM((2, N_DEV, 2, 8, 128), f32),
            pltpu.VMEM((2, 256, 256), jnp.bfloat16),
            pltpu.VMEM((2, 4, 8, 128), f32),
            pltpu.SemaphoreType.DMA((5,)),
            pltpu.SemaphoreType.DMA((5,)),
            pltpu.SemaphoreType.DMA((5,)),
        ],
        compiler_params=pltpu.CompilerParams(
            collective_id=0, has_side_effects=True, vmem_limit_bytes=24 * 1024 * 1024
        ),
        name="register",
    )(
        *(
            pltpu.with_memory_space_constraint(array, pltpu.HBM)
            for array in (
                amplitudes.reshape(2, N_DEV, 2, 8, 128),
                energies.reshape(N_DEV, 2, 8, 128),
                diagonal_angles,
                turn_angles,
            )
        )
    )
    return out.reshape(2, 16, 128, 128)


def solution(mesh):
    split = P(None, ("bank", "lane"), None, None)
    in_specs = (split, P(("bank", "lane"), None, None), P(), P())
    return jax.shard_map(body, mesh=mesh, in_specs=in_specs, out_specs=split, check_vma=False)
```

```python
import itertools

import jax
import jax.numpy as jnp
from jax import lax
from jax.experimental import pallas as pl
from jax.experimental.pallas import tpu as pltpu
from jax.sharding import PartitionSpec as P

N_DEV = 128
N_LANE = 16
BITS = 7


def place():
    return lax.axis_index("bank"), lax.axis_index("lane")


def hops(step):
    return min(step, 4 - step)


STEPS = sorted(
    (s for s in itertools.product(range(4), range(2), range(4), range(4)) if any(s)),
    key=lambda s: -hops(s[0]) - hops(s[2]) - hops(s[3]),
)


def others():
    bank, lane = place()
    x, core, z, y = bank // 2, lax.rem(bank, 2), lane // 4, lax.rem(lane, 4)
    xs = [lax.rem(x + s, 4) * 2 for s in range(4)]
    cores = [core, 1 - core]
    zs = [lax.rem(z + s, 4) * 4 for s in range(4)]
    ys = [lax.rem(y + s, 4) for s in range(4)]
    banks = {(i, j): xs[i] + cores[j] for i in range(4) for j in range(2)}
    lanes = {(i, j): zs[i] + ys[j] for i in range(4) for j in range(4)}
    found = []
    for sx, sc, sz, sy in STEPS:
        to_bank, to_lane = banks[sx, sc], lanes[sz, sy]
        found.append(((to_bank, to_lane), to_bank * N_LANE + to_lane))
    return found


def send_all(devices, pick_src, dst, send_sem, recv_sem):
    for device, index in devices:
        pltpu.make_async_remote_copy(
            src_ref=pick_src(index),
            dst_ref=dst,
            send_sem=send_sem,
            recv_sem=recv_sem,
            device_id=device,
            device_id_type=pl.DeviceIdType.MESH,
        ).start()


def wait_bytes(ref, sem):
    pltpu.make_async_copy(ref, ref, sem).wait()


def cos_sin(half):
    sq = half * half
    s = 1.0 / 6227020800.0
    for term in (-1.0 / 39916800.0, 1.0 / 362880.0, -1.0 / 5040.0, 1.0 / 120.0, -1.0 / 6.0):
        s = s * sq + term
    s = half + half * (sq * s)
    c = 1.0 / 479001600.0
    for term in (-1.0 / 3628800.0, 1.0 / 40320.0, -1.0 / 720.0, 1.0 / 24.0, -0.5):
        c = c * sq + term
    c = 1.0 + sq * c
    twice = s + s
    return 1.0 - twice * s, twice * c


def butterfly(tiles, tan):
    tiles = list(tiles)
    step = 1
    while step < len(tiles):
        for i in range(len(tiles)):
            if i & step:
                continue
            u, v = tiles[i], tiles[i + step]
            tiles[i] = u - tan * v
            tiles[i + step] = v + tan * u
        step *= 2
    return tiles


def rotate_phase(re, im, half):
    c, s = cos_sin(half)
    return re * c + im * s, im * c - re * s


def sublane_mix(values, tan):
    place_in = lax.broadcasted_iota(jnp.int32, values.shape, 1)
    for step in (4, 2, 1):
        upper = (place_in // step) % 2 == 1
        below = pltpu.roll(values, step, 1)
        other = below if step == 4 else jnp.where(upper, below, pltpu.roll(values, 8 - step, 1))
        values = values + jnp.where(upper, tan, -tan) * other
    return values


def lane_table(cos, sin, scale):
    row = lax.broadcasted_iota(jnp.int32, (128, 128), 0)
    col = lax.broadcasted_iota(jnp.int32, (128, 128), 1)
    table = jnp.broadcast_to(scale, (128, 128))
    for bit in range(BITS):
        r = (row // 2**bit) % 2
        c = (col // 2**bit) % 2
        table = table * jnp.where(r == c, cos, jnp.where(r > c, -sin, sin))
    high = table.astype(jnp.bfloat16)
    low = (table - high.astype(jnp.float32)).astype(jnp.bfloat16)
    both = jnp.concatenate([high, low], axis=1)
    return jnp.concatenate([both, both], axis=0)


def lane_mix(values, table):
    high = values.astype(jnp.bfloat16)
    low = (values - high.astype(jnp.float32)).astype(jnp.bfloat16)
    parts = jnp.concatenate([high, low], axis=1)
    out = jnp.dot(parts, table, preferred_element_type=jnp.float32)
    return out[:, :128] + out[:, 128:]


def kernel(amp, energy, diag_any, turn_any, out, diag, turn, a_in, e_in, e_rx, fwd, mid, back, fin, tables, tans, sems, sends, recvs):
    bank, lane = place()
    me = bank * N_LANE + lane
    scope = jax.named_scope

    get_e = pltpu.make_async_copy(energy, e_in, sems.at[0])
    get_a = pltpu.make_async_copy(amp, a_in, sems.at[1])
    small = [pltpu.make_async_copy(diag_any, diag, sems.at[2]), pltpu.make_async_copy(turn_any, turn, sems.at[3])]
    for get in [get_e, *small, get_a]:
        get.start()

    devices = others()
    barrier = pltpu.get_barrier_semaphore()
    with scope("signals"):
        for device, _ in devices:
            pl.semaphore_signal(barrier, 1, device_id=device, device_id_type=pl.DeviceIdType.MESH)

    with scope("tables"):
        for get in small:
            get.wait()
        cos, sin = cos_sin(turn[...] * 0.5)
        tan = sin / cos
        for layer in range(2):
            for group in range(4):
                tans[layer, group] = jnp.broadcast_to(tan[layer : layer + 1, group : group + 1], (8, 128))
            c = [cos[layer : layer + 1, g : g + 1] for g in range(4)]
            c12 = c[1] * c[2]
            c12_2 = c12 * c12
            c3_2 = c[3] * c[3]
            scale = c12_2 * c12_2 * c12_2 * c12 * c3_2 * c3_2
            tables[layer] = lane_table(c[0], sin[layer : layer + 1, 0:1], scale)

    with scope("wait_in"):
        get_e.wait()
        get_a.wait()
    with scope("barrier"):
        pl.semaphore_wait(barrier, N_DEV - 1)
    with scope("send_e"):
        send_all(devices, lambda i: e_in.at[i], e_rx.at[me], sends.at[5], recvs.at[5])
    e_rx[me] = e_in[me]

    def first(i, carry):
        at = pl.ds(i * 8, 8)
        angle = (diag[0:1, :] * 0.5).reshape(1, 1, 1, 128)
        half = e_in[at] * angle
        re, im = rotate_phase(a_in[0, at], a_in[1, at], half)
        values = jnp.concatenate([re, im], axis=0)
        mixed = lane_mix(values.reshape(256, 128), tables[0]).reshape(32, 8, 128)
        mixed = sublane_mix(mixed, tans[0, 1, 0:1, :].reshape(1, 1, 128))
        mixed = mixed.reshape(2, 16, 8, 128)
        tan1 = tans[0, 1]
        for part in range(2):
            tiles = butterfly([mixed[part, j] for j in range(16)], tan1)
            for j in range(16):
                a_in[part, i * 8 + j // 2, j % 2] = tiles[j]
        return carry

    with scope("first"):
        lax.fori_loop(0, 16, first, 0)

    tan2 = tans[0, 2]
    for k in range(2):

        def blocks(i, carry):
            part, row = i // 8, lax.rem(i, 8)
            tiles = butterfly([a_in[part, b * 8 + row, k] for b in range(16)], tan2)
            for b in range(16):
                fwd[k, b * 8 + row, part] = tiles[b]
            return carry

        with scope(f"blocks_{k}"):
            lax.fori_loop(0, 16, blocks, 0)
        with scope(f"send_f{k}"):
            send_all(devices, lambda i: fwd.at[k, i], mid.at[k, me], sends.at[k], recvs.at[k])
        mid[k, me] = fwd[k, me]

    with scope("wait_e"):
        wait_bytes(e_rx.at[pl.ds(0, N_DEV - 1)], recvs.at[5])
    for k in range(2):
        with scope(f"wait_m{k}"):
            wait_bytes(mid.at[k, pl.ds(0, N_DEV - 1)], recvs.at[k])

        def lanes_1(i, carry):
            b, part = i // 2, lax.rem(i, 2)
            tiles = butterfly([mid[k, b * 16 + l, part] for l in range(16)], tans[0, 3])
            for l in range(16):
                mid[k, b * 16 + l, part] = tiles[l]
            return carry

        def banks(l, carry):
            re = butterfly([mid[k, b * 16 + l, 0] for b in range(8)], tans[0, 2])
            im = butterfly([mid[k, b * 16 + l, 1] for b in range(8)], tans[0, 2])
            angle = diag[1:2, :] * 0.5
            for b in range(8):
                re[b], im[b] = rotate_phase(re[b], im[b], e_rx[b * 16 + l, k] * angle)
            re = butterfly(re, tans[1, 2])
            im = butterfly(im, tans[1, 2])
            for b in range(8):
                mid[k, b * 16 + l, 0] = re[b]
                mid[k, b * 16 + l, 1] = im[b]
            return carry

        def lanes_2(b, carry):
            both = []
            for part in range(2):
                tiles = butterfly([mid[k, b * 16 + l, part] for l in range(16)], tans[1, 3])
                both.append(jnp.stack(tiles))
            values = jnp.stack(both).reshape(256, 128)
            mixed = lane_mix(values, tables[1]).reshape(32, 8, 128)
            mixed = sublane_mix(mixed, tans[1, 1, 0:1, :].reshape(1, 1, 128))
            mixed = mixed.reshape(2, 16, 8, 128)
            for part in range(2):
                back[k, pl.ds(b * 16, 16), part] = mixed[part]
            return carry

        with scope(f"mid_{k}"):
            lax.fori_loop(0, 16, lanes_1, 0)
            lax.fori_loop(0, 16, banks, 0)
            lax.fori_loop(0, 8, lanes_2, 0)
        with scope(f"send_b{k}"):
            if k == 0:
                send_all(devices, lambda i: back.at[0, i], fin.at[0, me], sends.at[2], recvs.at[2])
            else:
                for part in range(2):
                    n = 3 + part
                    send_all(
                        devices, lambda i: back.at[1, i, part], fin.at[1, me, part], sends.at[n], recvs.at[n]
                    )
        fin[k, me] = back[k, me]

    for k in range(2):
        for part in range(2):
            with scope(f"wait_b{k}{part}"):
                if k == 1:
                    wait_bytes(fin.at[1, pl.ds(0, N_DEV - 1), part], recvs.at[3 + part])
                elif part == 0:
                    wait_bytes(fin.at[0, pl.ds(0, N_DEV - 1)], recvs.at[2])

            def rows(b, carry):
                tiles = butterfly([fin[k, b * 8 + r, part] for r in range(8)], tans[1, 1])
                for r in range(8):
                    fin[k, b * 8 + r, part] = tiles[r]
                return carry

            def last(r, carry):
                tiles = butterfly([fin[k, b * 8 + r, part] for b in range(16)], tans[1, 2])
                if k == 0:
                    for b in range(16):
                        fin[0, b * 8 + r, part] = tiles[b]
                else:
                    t = tans[1, 1]
                    for b in range(16):
                        u = fin[0, b * 8 + r, part]
                        v = tiles[b]
                        out[part, b * 8 + r, 0] = u - t * v
                        out[part, b * 8 + r, 1] = v + t * u
                return carry

            with scope(f"last_{k}{part}"):
                lax.fori_loop(0, 16, rows, 0)
                lax.fori_loop(0, 8, last, 0)

    wait_bytes(e_in.at[pl.ds(0, N_DEV - 1)], sends.at[5])
    for k in range(2):
        wait_bytes(fwd.at[k, pl.ds(0, N_DEV - 1)], sends.at[k])
    wait_bytes(back.at[0, pl.ds(0, N_DEV - 1)], sends.at[2])
    for part in range(2):
        wait_bytes(back.at[1, pl.ds(0, N_DEV - 1), part], sends.at[3 + part])


def body(amplitudes, energies, diagonal_angles, turn_angles):
    f32 = jnp.float32
    anywhere = pl.BlockSpec(memory_space=pl.ANY)
    vmem = pl.BlockSpec(memory_space=pltpu.VMEM)
    out = pl.pallas_call(
        kernel,
        out_shape=pltpu.VMEM((2, N_DEV, 2, 8, 128), f32),
        in_specs=[anywhere] * 4,
        out_specs=vmem,
        scratch_shapes=[
            pltpu.VMEM((2, 128), f32),
            pltpu.VMEM((2, 4), f32),
            pltpu.VMEM((2, N_DEV, 2, 8, 128), f32),
            pltpu.VMEM((N_DEV, 2, 8, 128), f32),
            pltpu.VMEM((N_DEV, 2, 8, 128), f32),
            pltpu.VMEM((2, N_DEV, 2, 8, 128), f32),
            pltpu.VMEM((2, N_DEV, 2, 8, 128), f32),
            pltpu.VMEM((2, N_DEV, 2, 8, 128), f32),
            pltpu.VMEM((2, N_DEV, 2, 8, 128), f32),
            pltpu.VMEM((2, 256, 256), jnp.bfloat16),
            pltpu.VMEM((2, 4, 8, 128), f32),
            pltpu.SemaphoreType.DMA((4,)),
            pltpu.SemaphoreType.DMA((6,)),
            pltpu.SemaphoreType.DMA((6,)),
        ],
        compiler_params=pltpu.CompilerParams(
            collective_id=0, has_side_effects=True, vmem_limit_bytes=24 * 1024 * 1024
        ),
        name="register",
    )(
        *(
            pltpu.with_memory_space_constraint(array, pltpu.HBM)
            for array in (
                amplitudes.reshape(2, N_DEV, 2, 8, 128),
                energies.reshape(N_DEV, 2, 8, 128),
                diagonal_angles,
                turn_angles,
            )
        )
    )
    return out.reshape(2, 16, 128, 128)


def solution(mesh):
    split = P(None, ("bank", "lane"), None, None)
    in_specs = (split, P(("bank", "lane"), None, None), P(), P())
    return jax.shard_map(body, mesh=mesh, in_specs=in_specs, out_specs=split, check_vma=False)
```

```python
import itertools

import jax
import jax.numpy as jnp
from jax import lax
from jax.experimental import pallas as pl
from jax.experimental.pallas import tpu as pltpu
from jax.sharding import PartitionSpec as P

N_DEV = 128
N_LANE = 16
BITS = 7


def place():
    return lax.axis_index("bank"), lax.axis_index("lane")


def hops(step):
    return min(step, 4 - step)


STEPS = sorted(
    (s for s in itertools.product(range(4), range(2), range(4), range(4)) if any(s)),
    key=lambda s: -hops(s[0]) - hops(s[2]) - hops(s[3]),
)


MIXED = sorted(STEPS, key=lambda s: (s[0] * 29 + s[1] * 53 + s[2] * 17 + s[3] * 71) * 37 % 127)


def lines(step):
    return int(any(step[:2])) + int(step[2] > 0) + int(step[3] > 0)


def along(step, line):
    part = [(step[0], step[1], 0, 0), (0, 0, step[2], 0), (0, 0, 0, step[3])]
    rest = [(0, 0, step[2], step[3]), (step[0], step[1], 0, step[3]), (step[0], step[1], step[2], 0)]
    return part[line], rest[line]


def reverse(step):
    return ((4 - step[0]) % 4, step[1], (4 - step[2]) % 4, (4 - step[3]) % 4)


RELAYED = [(s, (s[0] * 2 + s[1] + s[2] + s[3]) % 3) for s in MIXED if lines(s) == 3]


def spots():
    bank, lane = place()
    x, core, z, y = bank // 2, lax.rem(bank, 2), lane // 4, lax.rem(lane, 4)
    xs = [lax.rem(x + s, 4) * 2 for s in range(4)]
    cores = [core, 1 - core]
    zs = [lax.rem(z + s, 4) * 4 for s in range(4)]
    ys = [lax.rem(y + s, 4) for s in range(4)]
    banks = {(i, j): xs[i] + cores[j] for i in range(4) for j in range(2)}
    lanes = {(i, j): zs[i] + ys[j] for i in range(4) for j in range(4)}

    def spot(step):
        to_bank, to_lane = banks[step[:2]], lanes[step[2:]]
        return (to_bank, to_lane), to_bank * N_LANE + to_lane

    return spot


def send(src, dst, device, send_sem, recv_sem):
    pltpu.make_async_remote_copy(
        src_ref=src,
        dst_ref=dst,
        send_sem=send_sem,
        recv_sem=recv_sem,
        device_id=device,
        device_id_type=pl.DeviceIdType.MESH,
    ).start()


def send_all(devices, pick_src, dst, send_sem, recv_sem):
    for device, index in devices:
        send(pick_src(index), dst, device, send_sem, recv_sem)


def wait_bytes(ref, sem):
    pltpu.make_async_copy(ref, ref, sem).wait()


def cos_sin(half):
    sq = half * half
    s = 1.0 / 6227020800.0
    for term in (-1.0 / 39916800.0, 1.0 / 362880.0, -1.0 / 5040.0, 1.0 / 120.0, -1.0 / 6.0):
        s = s * sq + term
    s = half + half * (sq * s)
    c = 1.0 / 479001600.0
    for term in (-1.0 / 3628800.0, 1.0 / 40320.0, -1.0 / 720.0, 1.0 / 24.0, -0.5):
        c = c * sq + term
    c = 1.0 + sq * c
    twice = s + s
    return 1.0 - twice * s, twice * c


def butterfly(tiles, tan):
    tiles = list(tiles)
    step = 1
    while step < len(tiles):
        for i in range(len(tiles)):
            if i & step:
                continue
            u, v = tiles[i], tiles[i + step]
            tiles[i] = u - tan * v
            tiles[i + step] = v + tan * u
        step *= 2
    return tiles


def rotate_phase(re, im, half):
    c, s = cos_sin(half)
    return re * c + im * s, im * c - re * s


def sublane_mix(values, tan):
    place_in = lax.broadcasted_iota(jnp.int32, values.shape, 1)
    for step in (4, 2, 1):
        upper = (place_in // step) % 2 == 1
        below = pltpu.roll(values, step, 1)
        other = below if step == 4 else jnp.where(upper, below, pltpu.roll(values, 8 - step, 1))
        values = values + jnp.where(upper, tan, -tan) * other
    return values


def lane_table(cos, sin, scale):
    row = lax.broadcasted_iota(jnp.int32, (128, 128), 0)
    col = lax.broadcasted_iota(jnp.int32, (128, 128), 1)
    table = jnp.broadcast_to(scale, (128, 128))
    for bit in range(BITS):
        r = (row // 2**bit) % 2
        c = (col // 2**bit) % 2
        table = table * jnp.where(r == c, cos, jnp.where(r > c, -sin, sin))
    high = table.astype(jnp.bfloat16)
    low = (table - high.astype(jnp.float32)).astype(jnp.bfloat16)
    both = jnp.concatenate([high, low], axis=1)
    return jnp.concatenate([both, both], axis=0)


def lane_mix(values, table):
    high = values.astype(jnp.bfloat16)
    low = (values - high.astype(jnp.float32)).astype(jnp.bfloat16)
    parts = jnp.concatenate([high, low], axis=1)
    out = jnp.dot(parts, table, preferred_element_type=jnp.float32)
    return out[:, :128] + out[:, 128:]


def home_rows(src, dst, tan):
    def one(b, carry):
        tiles = butterfly([src[b * 8 + r] for r in range(8)], tan[0])
        for r in range(8):
            dst[b * 8 + r] = tiles[r]
        return carry

    lax.fori_loop(0, 16, one, 0)


def home_blocks(pick, pick_other, dst, r, tan):
    tiles = butterfly([pick(b * 8 + r) for b in range(16)], tan[1])
    for b in range(16):
        u, v = pick_other(b * 8 + r), tiles[b]
        dst[b, r, 0] = u - tan[0] * v
        dst[b, r, 1] = v + tan[0] * u


def finish(done, half_done, raw, tan, out, rows, stage, sems):
    copies = [pltpu.make_async_copy(done.at[pl.ds(i * 4, 4)], out.at[0, pl.ds(i * 4, 4)], sems.at[i]) for i in range(4)]
    for copy in copies:
        copy.start()
    home_rows(raw, rows, tan)
    for r in range(8):
        home_blocks(lambda d: rows[d], lambda d: half_done[d], stage, r, tan)
        if r % 2:
            copies.append(pltpu.make_async_copy(stage.at[:, pl.ds(r - 1, 2)], out.at[1, :, pl.ds(r - 1, 2)], sems.at[4 + r // 2]))
            copies[-1].start()
    for copy in copies:
        copy.wait()


def kernel(amp, energy, diag_any, turn_any, done, half_done, raw, tan_out, diag, turn, a_in, e_in, e_rx, relay, fwd, mid, back, fin, fin_1, tables, tans, sems, sends, recvs, met):
    bank, lane = place()
    me = bank * N_LANE + lane
    scope = jax.named_scope
    late = [fin_1, raw]

    get_e = pltpu.make_async_copy(energy, e_in, sems.at[0])
    get_a = pltpu.make_async_copy(amp, a_in, sems.at[1])
    small = [pltpu.make_async_copy(diag_any, diag, sems.at[2]), pltpu.make_async_copy(turn_any, turn, sems.at[3])]
    for get in [get_e, *small, get_a]:
        get.start()

    spot = spots()
    devices = [spot(step) for step in STEPS]
    mixed = [spot(step) for step in MIXED]
    near = [spot(step)[0] for step in MIXED if lines(step) == 1]
    rounds = [pltpu.get_barrier_semaphore(), met.at[0], met.at[1]]

    def signal(n):
        for device in near:
            pl.semaphore_signal(rounds[n], 1, device_id=device, device_id_type=pl.DeviceIdType.MESH)

    def meet(n):
        with scope(f"meet_{n}"):
            pl.semaphore_wait(rounds[n], len(near))
        if n < 2:
            signal(n + 1)

    def send_e(n):
        some = [spot(step) for step in MIXED if lines(step) == n]
        send_all(some, lambda i: e_in.at[i], e_rx.at[me], sends.at[5], recvs.at[5])

    signal(0)
    with scope("wait_in"):
        get_e.wait()
    meet(0)
    with scope("send_e0"):
        send_e(1)
        for j, (step, line) in enumerate(RELAYED):
            device, _ = spot(along(step, line)[0])
            send(e_in.at[spot(step)[1]], relay.at[j], device, sends.at[5], recvs.at[6])
    e_rx[me] = e_in[me]

    with scope("tables"):
        for get in [*small, get_a]:
            get.wait()
        cos, sin = cos_sin(turn[...] * 0.5)
        tan = sin / cos
        for layer in range(2):
            for group in range(4):
                tans[layer, group] = jnp.broadcast_to(tan[layer : layer + 1, group : group + 1], (8, 128))
            c = [cos[layer : layer + 1, g : g + 1] for g in range(4)]
            c12 = c[1] * c[2]
            c12_2 = c12 * c12
            c3_2 = c[3] * c[3]
            scale = c12_2 * c12_2 * c12_2 * c12 * c3_2 * c3_2
            tables[layer] = lane_table(c[0], sin[layer : layer + 1, 0:1], scale)

    def first(i, carry):
        at = pl.ds(i * 8, 8)
        angle = (diag[0:1, :] * 0.5).reshape(1, 1, 1, 128)
        half = e_in[at] * angle
        re, im = rotate_phase(a_in[0, at], a_in[1, at], half)
        values = jnp.concatenate([re, im], axis=0)
        mixed = lane_mix(values.reshape(256, 128), tables[0]).reshape(32, 8, 128)
        mixed = sublane_mix(mixed, tans[0, 1, 0:1, :].reshape(1, 1, 128))
        mixed = mixed.reshape(2, 16, 8, 128)
        tan1 = tans[0, 1]
        for part in range(2):
            tiles = butterfly([mixed[part, j] for j in range(16)], tan1)
            for j in range(16):
                a_in[part, i * 8 + j // 2, j % 2] = tiles[j]
        return carry

    with scope("first_0"):
        lax.fori_loop(0, 4, first, 0)
    meet(1)
    send_e(2)
    with scope("first_1"):
        lax.fori_loop(4, 8, first, 0)
    with scope("wait_r"):
        wait_bytes(relay, recvs.at[6])
    with scope("relay"):
        for j, (step, line) in enumerate(RELAYED):
            part, rest = along(step, line)
            send(relay.at[j], e_rx.at[spot(reverse(part))[1]], spot(rest)[0], sends.at[6], recvs.at[5])
    with scope("first_2"):
        lax.fori_loop(8, 16, first, 0)
    meet(2)

    tan2 = tans[0, 2]
    for k in range(2):

        def blocks(i, carry):
            part, row = i // 8, lax.rem(i, 8)
            tiles = butterfly([a_in[part, b * 8 + row, k] for b in range(16)], tan2)
            for b in range(16):
                fwd[k, b * 8 + row, part] = tiles[b]
            return carry

        with scope(f"blocks_{k}"):
            lax.fori_loop(0, 16, blocks, 0)
        with scope(f"send_f{k}"):
            send_all(mixed, lambda i: fwd.at[k, i], mid.at[k, me], sends.at[k], recvs.at[k])
        mid[k, me] = fwd[k, me]

    with scope("wait_e"):
        wait_bytes(e_rx.at[pl.ds(0, N_DEV - 1)], recvs.at[5])
    for k in range(2):
        with scope(f"wait_m{k}"):
            wait_bytes(mid.at[k, pl.ds(0, N_DEV - 1)], recvs.at[k])

        def lanes_1(i, carry):
            b, part = i // 2, lax.rem(i, 2)
            tiles = butterfly([mid[k, b * 16 + l, part] for l in range(16)], tans[0, 3])
            for l in range(16):
                mid[k, b * 16 + l, part] = tiles[l]
            return carry

        def banks(l, carry):
            re = butterfly([mid[k, b * 16 + l, 0] for b in range(8)], tans[0, 2])
            im = butterfly([mid[k, b * 16 + l, 1] for b in range(8)], tans[0, 2])
            angle = diag[1:2, :] * 0.5
            for b in range(8):
                re[b], im[b] = rotate_phase(re[b], im[b], e_rx[b * 16 + l, k] * angle)
            re = butterfly(re, tans[1, 2])
            im = butterfly(im, tans[1, 2])
            for b in range(8):
                mid[k, b * 16 + l, 0] = re[b]
                mid[k, b * 16 + l, 1] = im[b]
            return carry

        def lanes_2(b, carry):
            both = []
            for part in range(2):
                tiles = butterfly([mid[k, b * 16 + l, part] for l in range(16)], tans[1, 3])
                both.append(jnp.stack(tiles))
            values = jnp.stack(both).reshape(256, 128)
            mixed = lane_mix(values, tables[1]).reshape(32, 8, 128)
            mixed = sublane_mix(mixed, tans[1, 1, 0:1, :].reshape(1, 1, 128))
            mixed = mixed.reshape(2, 16, 8, 128)
            for part in range(2):
                back[k, pl.ds(b * 16, 16), part] = mixed[part]
            return carry

        with scope(f"mid_{k}"):
            lax.fori_loop(0, 16, lanes_1, 0)
            lax.fori_loop(0, 16, banks, 0)
            lax.fori_loop(0, 8, lanes_2, 0)
        with scope(f"send_b{k}"):
            if k == 0:
                send_all(mixed, lambda i: back.at[0, i], fin.at[me], sends.at[2], recvs.at[2])
            else:
                for part in range(2):
                    n = 3 + part
                    send_all(
                        devices, lambda i: back.at[1, i, part], late[part].at[me], sends.at[n], recvs.at[n]
                    )
        if k == 0:
            fin[me] = back[0, me]
        else:
            for part in range(2):
                late[part][me] = back[1, me, part]

    with scope("wait_b0"):
        wait_bytes(fin.at[pl.ds(0, N_DEV - 1)], recvs.at[2])
    tan_out[0] = tans[1, 1]
    tan_out[1] = tans[1, 2]
    with scope("last_0"):
        for part in range(2):
            home_rows(fin.at[:, part], fin.at[:, part], tan_out)

            def last(r, carry):
                tiles = butterfly([fin[b * 8 + r, part] for b in range(16)], tan_out[1])
                for b in range(16):
                    if part == 0:
                        fin[b * 8 + r, 0] = tiles[b]
                    else:
                        half_done[b * 8 + r] = tiles[b]
                return carry

            lax.fori_loop(0, 8, last, 0)
    with scope("wait_b10"):
        wait_bytes(fin_1.at[pl.ds(0, N_DEV - 1)], recvs.at[3])
    with scope("last_10"):
        home_rows(fin_1, fin_1, tan_out)

        def last_0(r, carry):
            home_blocks(lambda d: fin_1[d], lambda d: fin[d, 0], done, r, tan_out)
            return carry

        lax.fori_loop(0, 8, last_0, 0)
    with scope("wait_b11"):
        wait_bytes(raw.at[pl.ds(0, N_DEV - 1)], recvs.at[4])

    wait_bytes(e_in.at[pl.ds(0, N_DEV - 1)], sends.at[5])
    wait_bytes(relay, sends.at[6])
    for k in range(2):
        wait_bytes(fwd.at[k, pl.ds(0, N_DEV - 1)], sends.at[k])
    wait_bytes(back.at[0, pl.ds(0, N_DEV - 1)], sends.at[2])
    for part in range(2):
        wait_bytes(back.at[1, pl.ds(0, N_DEV - 1), part], sends.at[3 + part])


def body(amplitudes, energies, diagonal_angles, turn_angles):
    f32 = jnp.float32
    anywhere = pl.BlockSpec(memory_space=pl.ANY)
    vmem = pl.BlockSpec(memory_space=pltpu.VMEM)
    done, half_done, raw, tan = pl.pallas_call(
        kernel,
        out_shape=(
            pltpu.VMEM((16, 8, 2, 8, 128), f32),
            pltpu.VMEM((N_DEV, 8, 128), f32),
            pltpu.VMEM((N_DEV, 8, 128), f32),
            pltpu.VMEM((2, 8, 128), f32),
        ),
        in_specs=[anywhere] * 4,
        out_specs=(vmem,) * 4,
        scratch_shapes=[
            pltpu.VMEM((2, 128), f32),
            pltpu.VMEM((2, 4), f32),
            pltpu.VMEM((2, N_DEV, 2, 8, 128), f32),
            pltpu.VMEM((N_DEV, 2, 8, 128), f32),
            pltpu.VMEM((N_DEV, 2, 8, 128), f32),
            pltpu.VMEM((len(RELAYED), 2, 8, 128), f32),
            pltpu.VMEM((2, N_DEV, 2, 8, 128), f32),
            pltpu.VMEM((2, N_DEV, 2, 8, 128), f32),
            pltpu.VMEM((2, N_DEV, 2, 8, 128), f32),
            pltpu.VMEM((N_DEV, 2, 8, 128), f32),
            pltpu.VMEM((N_DEV, 8, 128), f32),
            pltpu.VMEM((2, 256, 256), jnp.bfloat16),
            pltpu.VMEM((2, 4, 8, 128), f32),
            pltpu.SemaphoreType.DMA((4,)),
            pltpu.SemaphoreType.DMA((7,)),
            pltpu.SemaphoreType.DMA((7,)),
            pltpu.SemaphoreType.REGULAR((2,)),
        ],
        compiler_params=pltpu.CompilerParams(
            collective_id=0, has_side_effects=True, vmem_limit_bytes=24 * 1024 * 1024
        ),
        name="register",
    )(
        *(
            pltpu.with_memory_space_constraint(array, pltpu.HBM)
            for array in (
                amplitudes.reshape(2, N_DEV, 2, 8, 128),
                energies.reshape(N_DEV, 2, 8, 128),
                diagonal_angles,
                turn_angles,
            )
        )
    )
    out = pl.pallas_call(
        finish,
        out_shape=jax.ShapeDtypeStruct((2, 16, 8, 2, 8, 128), f32),
        in_specs=[vmem] * 4,
        out_specs=anywhere,
        scratch_shapes=[
            pltpu.VMEM((N_DEV, 8, 128), f32),
            pltpu.VMEM((16, 8, 2, 8, 128), f32),
            pltpu.SemaphoreType.DMA((8,)),
        ],
        compiler_params=pltpu.CompilerParams(vmem_limit_bytes=8 * 1024 * 1024),
        name="finish",
    )(done, half_done, raw, tan)
    return out.reshape(2, 16, 128, 128)


def solution(mesh):
    split = P(None, ("bank", "lane"), None, None)
    in_specs = (split, P(("bank", "lane"), None, None), P(), P())
    return jax.shard_map(body, mesh=mesh, in_specs=in_specs, out_specs=split, check_vma=False)
```

```python
import itertools

import jax
import jax.numpy as jnp
from jax import lax
from jax.experimental import pallas as pl
from jax.experimental.pallas import tpu as pltpu
from jax.sharding import PartitionSpec as P

N_DEV = 128
N_LANE = 16
BITS = 7


def place():
    return lax.axis_index("bank"), lax.axis_index("lane")


def hops(step):
    return min(step, 4 - step)


STEPS = sorted(
    (s for s in itertools.product(range(4), range(2), range(4), range(4)) if any(s)),
    key=lambda s: -hops(s[0]) - hops(s[2]) - hops(s[3]),
)


MIXED = sorted(STEPS, key=lambda s: (s[0] * 29 + s[1] * 53 + s[2] * 17 + s[3] * 71) * 37 % 127)


def lines(step):
    return int(any(step[:2])) + int(step[2] > 0) + int(step[3] > 0)


def along(step, line):
    part = [(step[0], step[1], 0, 0), (0, 0, step[2], 0), (0, 0, 0, step[3])]
    rest = [(0, 0, step[2], step[3]), (step[0], step[1], 0, step[3]), (step[0], step[1], step[2], 0)]
    return part[line], rest[line]


def reverse(step):
    return ((4 - step[0]) % 4, step[1], (4 - step[2]) % 4, (4 - step[3]) % 4)


RELAYED = [(s, (s[0] * 2 + s[1] + s[2] + s[3]) % 3) for s in MIXED if lines(s) == 3]


def spots():
    bank, lane = place()
    x, core, z, y = bank // 2, lax.rem(bank, 2), lane // 4, lax.rem(lane, 4)
    xs = [lax.rem(x + s, 4) * 2 for s in range(4)]
    cores = [core, 1 - core]
    zs = [lax.rem(z + s, 4) * 4 for s in range(4)]
    ys = [lax.rem(y + s, 4) for s in range(4)]
    banks = {(i, j): xs[i] + cores[j] for i in range(4) for j in range(2)}
    lanes = {(i, j): zs[i] + ys[j] for i in range(4) for j in range(4)}

    def spot(step):
        to_bank, to_lane = banks[step[:2]], lanes[step[2:]]
        return (to_bank, to_lane), to_bank * N_LANE + to_lane

    return spot


def send(src, dst, device, send_sem, recv_sem):
    pltpu.make_async_remote_copy(
        src_ref=src,
        dst_ref=dst,
        send_sem=send_sem,
        recv_sem=recv_sem,
        device_id=device,
        device_id_type=pl.DeviceIdType.MESH,
    ).start()


def send_all(devices, pick_src, dst, send_sem, recv_sem):
    for device, index in devices:
        send(pick_src(index), dst, device, send_sem, recv_sem)


def wait_bytes(ref, sem):
    pltpu.make_async_copy(ref, ref, sem).wait()


def cos_sin(half):
    sq = half * half
    s = 1.0 / 6227020800.0
    for term in (-1.0 / 39916800.0, 1.0 / 362880.0, -1.0 / 5040.0, 1.0 / 120.0, -1.0 / 6.0):
        s = s * sq + term
    s = half + half * (sq * s)
    c = 1.0 / 479001600.0
    for term in (-1.0 / 3628800.0, 1.0 / 40320.0, -1.0 / 720.0, 1.0 / 24.0, -0.5):
        c = c * sq + term
    c = 1.0 + sq * c
    twice = s + s
    return 1.0 - twice * s, twice * c


def butterfly(tiles, tan):
    tiles = list(tiles)
    step = 1
    while step < len(tiles):
        for i in range(len(tiles)):
            if i & step:
                continue
            u, v = tiles[i], tiles[i + step]
            tiles[i] = u - tan * v
            tiles[i + step] = v + tan * u
        step *= 2
    return tiles


def rotate_phase(re, im, half):
    c, s = cos_sin(half)
    return re * c + im * s, im * c - re * s


def sublane_mix(values, tan):
    place_in = lax.broadcasted_iota(jnp.int32, values.shape, 1)
    for step in (4, 2, 1):
        upper = (place_in // step) % 2 == 1
        below = pltpu.roll(values, step, 1)
        other = below if step == 4 else jnp.where(upper, below, pltpu.roll(values, 8 - step, 1))
        values = values + jnp.where(upper, tan, -tan) * other
    return values


def lane_table(cos, sin, scale):
    row = lax.broadcasted_iota(jnp.int32, (128, 128), 0)
    col = lax.broadcasted_iota(jnp.int32, (128, 128), 1)
    table = jnp.broadcast_to(scale, (128, 128))
    for bit in range(BITS):
        r = (row // 2**bit) % 2
        c = (col // 2**bit) % 2
        table = table * jnp.where(r == c, cos, jnp.where(r > c, -sin, sin))
    high = table.astype(jnp.bfloat16)
    low = (table - high.astype(jnp.float32)).astype(jnp.bfloat16)
    both = jnp.concatenate([high, low], axis=1)
    return jnp.concatenate([both, both], axis=0)


def lane_mix(values, table):
    high = values.astype(jnp.bfloat16)
    low = (values - high.astype(jnp.float32)).astype(jnp.bfloat16)
    parts = jnp.concatenate([high, low], axis=1)
    out = jnp.dot(parts, table, preferred_element_type=jnp.float32)
    return out[:, :128] + out[:, 128:]


def home_rows(src, dst, tan):
    def one(b, carry):
        tiles = butterfly([src[b * 8 + r] for r in range(8)], tan[0])
        for r in range(8):
            dst[b * 8 + r] = tiles[r]
        return carry

    lax.fori_loop(0, 16, one, 0, unroll=4)


def home_blocks(pick, pick_other, dst, r, tan):
    tiles = butterfly([pick(b * 8 + r) for b in range(16)], tan[1])
    for b in range(16):
        u, v = pick_other(b * 8 + r), tiles[b]
        dst[b, r, 0] = u - tan[0] * v
        dst[b, r, 1] = v + tan[0] * u


def finish(done, half_done, raw, tan, out, rows, stage, sems):
    copies = [pltpu.make_async_copy(done.at[pl.ds(i * 4, 4)], out.at[0, pl.ds(i * 4, 4)], sems.at[i]) for i in range(4)]
    for copy in copies:
        copy.start()
    home_rows(raw, rows, tan)
    for r in range(8):
        home_blocks(lambda d: rows[d], lambda d: half_done[d], stage, r, tan)
        if r % 2:
            copies.append(pltpu.make_async_copy(stage.at[:, pl.ds(r - 1, 2)], out.at[1, :, pl.ds(r - 1, 2)], sems.at[4 + r // 2]))
            copies[-1].start()
    for copy in copies:
        copy.wait()


def kernel(amp, energy, diag_any, turn_any, done, half_done, raw, tan_out, diag, turn, a_in, e_in, e_rx, relay, fwd, mid, back, fin, fin_1, tables, tans, sems, sends, recvs, met):
    bank, lane = place()
    me = bank * N_LANE + lane
    scope = jax.named_scope
    late = [fin_1, raw]

    get_e = pltpu.make_async_copy(energy, e_in, sems.at[0])
    get_a = pltpu.make_async_copy(amp, a_in, sems.at[1])
    small = [pltpu.make_async_copy(diag_any, diag, sems.at[2]), pltpu.make_async_copy(turn_any, turn, sems.at[3])]
    for get in [get_e, *small, get_a]:
        get.start()

    spot = spots()
    devices = [spot(step) for step in STEPS]
    mixed = [spot(step) for step in MIXED]
    near = [spot(step)[0] for step in MIXED if lines(step) == 1]
    rounds = [pltpu.get_barrier_semaphore(), met.at[0], met.at[1]]

    def signal(n):
        for device in near:
            pl.semaphore_signal(rounds[n], 1, device_id=device, device_id_type=pl.DeviceIdType.MESH)

    def meet(n):
        with scope(f"meet_{n}"):
            pl.semaphore_wait(rounds[n], len(near))
        if n < 2:
            signal(n + 1)

    def send_e(n):
        some = [spot(step) for step in MIXED if lines(step) == n]
        send_all(some, lambda i: e_in.at[i], e_rx.at[me], sends.at[5], recvs.at[5])

    signal(0)
    with scope("wait_in"):
        get_e.wait()
    meet(0)
    with scope("send_e0"):
        send_e(1)
        for j, (step, line) in enumerate(RELAYED):
            device, _ = spot(along(step, line)[0])
            send(e_in.at[spot(step)[1]], relay.at[j], device, sends.at[5], recvs.at[6])
    e_rx[me] = e_in[me]

    with scope("tables"):
        for get in [*small, get_a]:
            get.wait()
        cos, sin = cos_sin(turn[...] * 0.5)
        tan = sin / cos
        for layer in range(2):
            for group in range(4):
                tans[layer, group] = jnp.broadcast_to(tan[layer : layer + 1, group : group + 1], (8, 128))
            c = [cos[layer : layer + 1, g : g + 1] for g in range(4)]
            c12 = c[1] * c[2]
            c12_2 = c12 * c12
            c3_2 = c[3] * c[3]
            scale = c12_2 * c12_2 * c12_2 * c12 * c3_2 * c3_2
            tables[layer] = lane_table(c[0], sin[layer : layer + 1, 0:1], scale)

    def first(i, carry):
        at = pl.ds(i * 8, 8)
        angle = (diag[0:1, :] * 0.5).reshape(1, 1, 1, 128)
        half = e_in[at] * angle
        re, im = rotate_phase(a_in[0, at], a_in[1, at], half)
        values = jnp.concatenate([re, im], axis=0)
        mixed = lane_mix(values.reshape(256, 128), tables[0]).reshape(32, 8, 128)
        mixed = sublane_mix(mixed, tans[0, 1, 0:1, :].reshape(1, 1, 128))
        mixed = mixed.reshape(2, 16, 8, 128)
        tan1 = tans[0, 1]
        for part in range(2):
            tiles = butterfly([mixed[part, j] for j in range(16)], tan1)
            for j in range(16):
                a_in[part, i * 8 + j // 2, j % 2] = tiles[j]
        return carry

    with scope("first_0"):
        lax.fori_loop(0, 4, first, 0, unroll=2)
    meet(1)
    send_e(2)
    with scope("first_1"):
        lax.fori_loop(4, 8, first, 0, unroll=2)
    with scope("wait_r"):
        wait_bytes(relay, recvs.at[6])
    with scope("relay"):
        for j, (step, line) in enumerate(RELAYED):
            part, rest = along(step, line)
            send(relay.at[j], e_rx.at[spot(reverse(part))[1]], spot(rest)[0], sends.at[6], recvs.at[5])
    with scope("first_2"):
        lax.fori_loop(8, 16, first, 0, unroll=2)
    meet(2)

    tan2 = tans[0, 2]
    for k in range(2):

        def blocks(i, carry):
            part, row = i // 8, lax.rem(i, 8)
            tiles = butterfly([a_in[part, b * 8 + row, k] for b in range(16)], tan2)
            for b in range(16):
                fwd[k, b * 8 + row, part] = tiles[b]
            return carry

        with scope(f"blocks_{k}"):
            lax.fori_loop(0, 16, blocks, 0, unroll=2)
        with scope(f"send_f{k}"):
            send_all(mixed, lambda i: fwd.at[k, i], mid.at[k, me], sends.at[k], recvs.at[k])
        mid[k, me] = fwd[k, me]

    with scope("wait_e"):
        wait_bytes(e_rx.at[pl.ds(0, N_DEV - 1)], recvs.at[5])
    for k in range(2):
        with scope(f"wait_m{k}"):
            wait_bytes(mid.at[k, pl.ds(0, N_DEV - 1)], recvs.at[k])

        def lanes_1(i, carry):
            b, part = i // 2, lax.rem(i, 2)
            tiles = butterfly([mid[k, b * 16 + l, part] for l in range(16)], tans[0, 3])
            for l in range(16):
                mid[k, b * 16 + l, part] = tiles[l]
            return carry

        def banks(l, carry):
            re = butterfly([mid[k, b * 16 + l, 0] for b in range(8)], tans[0, 2])
            im = butterfly([mid[k, b * 16 + l, 1] for b in range(8)], tans[0, 2])
            angle = diag[1:2, :] * 0.5
            for b in range(8):
                re[b], im[b] = rotate_phase(re[b], im[b], e_rx[b * 16 + l, k] * angle)
            re = butterfly(re, tans[1, 2])
            im = butterfly(im, tans[1, 2])
            for b in range(8):
                mid[k, b * 16 + l, 0] = re[b]
                mid[k, b * 16 + l, 1] = im[b]
            return carry

        def lanes_2(b, carry):
            both = []
            for part in range(2):
                tiles = butterfly([mid[k, b * 16 + l, part] for l in range(16)], tans[1, 3])
                both.append(jnp.stack(tiles))
            values = jnp.stack(both).reshape(256, 128)
            mixed = lane_mix(values, tables[1]).reshape(32, 8, 128)
            mixed = sublane_mix(mixed, tans[1, 1, 0:1, :].reshape(1, 1, 128))
            mixed = mixed.reshape(2, 16, 8, 128)
            for part in range(2):
                back[k, pl.ds(b * 16, 16), part] = mixed[part]
            return carry

        with scope(f"mid_{k}"):
            lax.fori_loop(0, 16, lanes_1, 0, unroll=2)
            lax.fori_loop(0, 16, banks, 0, unroll=2)
            lax.fori_loop(0, 8, lanes_2, 0, unroll=2)
        with scope(f"send_b{k}"):
            if k == 0:
                send_all(mixed, lambda i: back.at[0, i], fin.at[me], sends.at[2], recvs.at[2])
            else:
                for part in range(2):
                    n = 3 + part
                    send_all(
                        devices, lambda i: back.at[1, i, part], late[part].at[me], sends.at[n], recvs.at[n]
                    )
        if k == 0:
            fin[me] = back[0, me]
        else:
            for part in range(2):
                late[part][me] = back[1, me, part]

    with scope("wait_b0"):
        wait_bytes(fin.at[pl.ds(0, N_DEV - 1)], recvs.at[2])
    tan_out[0] = tans[1, 1]
    tan_out[1] = tans[1, 2]
    with scope("last_0"):
        for part in range(2):
            home_rows(fin.at[:, part], fin.at[:, part], tan_out)

            def last(r, carry):
                tiles = butterfly([fin[b * 8 + r, part] for b in range(16)], tan_out[1])
                for b in range(16):
                    if part == 0:
                        fin[b * 8 + r, 0] = tiles[b]
                    else:
                        half_done[b * 8 + r] = tiles[b]
                return carry

            lax.fori_loop(0, 8, last, 0, unroll=2)
    with scope("wait_b10"):
        wait_bytes(fin_1.at[pl.ds(0, N_DEV - 1)], recvs.at[3])
    with scope("last_10"):
        home_rows(fin_1, fin_1, tan_out)

        def last_0(r, carry):
            home_blocks(lambda d: fin_1[d], lambda d: fin[d, 0], done, r, tan_out)
            return carry

        lax.fori_loop(0, 8, last_0, 0, unroll=2)
    with scope("wait_b11"):
        wait_bytes(raw.at[pl.ds(0, N_DEV - 1)], recvs.at[4])

    wait_bytes(e_in.at[pl.ds(0, N_DEV - 1)], sends.at[5])
    wait_bytes(relay, sends.at[6])
    for k in range(2):
        wait_bytes(fwd.at[k, pl.ds(0, N_DEV - 1)], sends.at[k])
    wait_bytes(back.at[0, pl.ds(0, N_DEV - 1)], sends.at[2])
    for part in range(2):
        wait_bytes(back.at[1, pl.ds(0, N_DEV - 1), part], sends.at[3 + part])


def body(amplitudes, energies, diagonal_angles, turn_angles):
    f32 = jnp.float32
    anywhere = pl.BlockSpec(memory_space=pl.ANY)
    vmem = pl.BlockSpec(memory_space=pltpu.VMEM)
    done, half_done, raw, tan = pl.pallas_call(
        kernel,
        out_shape=(
            pltpu.VMEM((16, 8, 2, 8, 128), f32),
            pltpu.VMEM((N_DEV, 8, 128), f32),
            pltpu.VMEM((N_DEV, 8, 128), f32),
            pltpu.VMEM((2, 8, 128), f32),
        ),
        in_specs=[anywhere] * 4,
        out_specs=(vmem,) * 4,
        scratch_shapes=[
            pltpu.VMEM((2, 128), f32),
            pltpu.VMEM((2, 4), f32),
            pltpu.VMEM((2, N_DEV, 2, 8, 128), f32),
            pltpu.VMEM((N_DEV, 2, 8, 128), f32),
            pltpu.VMEM((N_DEV, 2, 8, 128), f32),
            pltpu.VMEM((len(RELAYED), 2, 8, 128), f32),
            pltpu.VMEM((2, N_DEV, 2, 8, 128), f32),
            pltpu.VMEM((2, N_DEV, 2, 8, 128), f32),
            pltpu.VMEM((2, N_DEV, 2, 8, 128), f32),
            pltpu.VMEM((N_DEV, 2, 8, 128), f32),
            pltpu.VMEM((N_DEV, 8, 128), f32),
            pltpu.VMEM((2, 256, 256), jnp.bfloat16),
            pltpu.VMEM((2, 4, 8, 128), f32),
            pltpu.SemaphoreType.DMA((4,)),
            pltpu.SemaphoreType.DMA((7,)),
            pltpu.SemaphoreType.DMA((7,)),
            pltpu.SemaphoreType.REGULAR((2,)),
        ],
        compiler_params=pltpu.CompilerParams(
            collective_id=0, has_side_effects=True, vmem_limit_bytes=24 * 1024 * 1024
        ),
        name="register",
    )(
        *(
            pltpu.with_memory_space_constraint(array, pltpu.HBM)
            for array in (
                amplitudes.reshape(2, N_DEV, 2, 8, 128),
                energies.reshape(N_DEV, 2, 8, 128),
                diagonal_angles,
                turn_angles,
            )
        )
    )
    out = pl.pallas_call(
        finish,
        out_shape=jax.ShapeDtypeStruct((2, 16, 8, 2, 8, 128), f32),
        in_specs=[vmem] * 4,
        out_specs=anywhere,
        scratch_shapes=[
            pltpu.VMEM((N_DEV, 8, 128), f32),
            pltpu.VMEM((16, 8, 2, 8, 128), f32),
            pltpu.SemaphoreType.DMA((8,)),
        ],
        compiler_params=pltpu.CompilerParams(vmem_limit_bytes=8 * 1024 * 1024),
        name="finish",
    )(done, half_done, raw, tan)
    return out.reshape(2, 16, 128, 128)


def solution(mesh):
    split = P(None, ("bank", "lane"), None, None)
    in_specs = (split, P(("bank", "lane"), None, None), P(), P())
    return jax.shard_map(body, mesh=mesh, in_specs=in_specs, out_specs=split, check_vma=False)
```

```python
import itertools

import jax
import jax.numpy as jnp
from jax import lax
from jax.experimental import pallas as pl
from jax.experimental.pallas import tpu as pltpu
from jax.sharding import PartitionSpec as P

N_DEV = 128
N_LANE = 16
BITS = 7


def place():
    return lax.axis_index("bank"), lax.axis_index("lane")


def hops(step):
    return min(step, 4 - step)


STEPS = sorted(
    (s for s in itertools.product(range(4), range(2), range(4), range(4)) if any(s)),
    key=lambda s: -hops(s[0]) - hops(s[2]) - hops(s[3]),
)


MIXED = sorted(STEPS, key=lambda s: (s[0] * 45 + s[1] * 91 + s[2] * 23 + s[3] * 103) * 61 % 127)


def lines(step):
    return int(any(step[:2])) + int(step[2] > 0) + int(step[3] > 0)


def along(step, line):
    part = [(step[0], step[1], 0, 0), (0, 0, step[2], 0), (0, 0, 0, step[3])]
    rest = [(0, 0, step[2], step[3]), (step[0], step[1], 0, step[3]), (step[0], step[1], step[2], 0)]
    return part[line], rest[line]


def reverse(step):
    return ((4 - step[0]) % 4, step[1], (4 - step[2]) % 4, (4 - step[3]) % 4)


RELAYED = [(s, (s[0] * 2 + s[1] + s[2] + s[3]) % 3) for s in MIXED if lines(s) == 3]


def spots():
    bank, lane = place()
    x, core, z, y = bank // 2, lax.rem(bank, 2), lane // 4, lax.rem(lane, 4)
    xs = [lax.rem(x + s, 4) * 2 for s in range(4)]
    cores = [core, 1 - core]
    zs = [lax.rem(z + s, 4) * 4 for s in range(4)]
    ys = [lax.rem(y + s, 4) for s in range(4)]
    banks = {(i, j): xs[i] + cores[j] for i in range(4) for j in range(2)}
    lanes = {(i, j): zs[i] + ys[j] for i in range(4) for j in range(4)}

    def spot(step):
        to_bank, to_lane = banks[step[:2]], lanes[step[2:]]
        return (to_bank, to_lane), to_bank * N_LANE + to_lane

    return spot


def send(src, dst, device, send_sem, recv_sem):
    pltpu.make_async_remote_copy(
        src_ref=src,
        dst_ref=dst,
        send_sem=send_sem,
        recv_sem=recv_sem,
        device_id=device,
        device_id_type=pl.DeviceIdType.MESH,
    ).start()


def send_all(devices, pick_src, dst, send_sem, recv_sem):
    for device, index in devices:
        send(pick_src(index), dst, device, send_sem, recv_sem)


def wait_bytes(ref, sem):
    pltpu.make_async_copy(ref, ref, sem).wait()


def cos_sin(half):
    sq = half * half
    s = 1.0 / 6227020800.0
    for term in (-1.0 / 39916800.0, 1.0 / 362880.0, -1.0 / 5040.0, 1.0 / 120.0, -1.0 / 6.0):
        s = s * sq + term
    s = half + half * (sq * s)
    c = 1.0 / 479001600.0
    for term in (-1.0 / 3628800.0, 1.0 / 40320.0, -1.0 / 720.0, 1.0 / 24.0, -0.5):
        c = c * sq + term
    c = 1.0 + sq * c
    twice = s + s
    return 1.0 - twice * s, twice * c


def butterfly(tiles, tan):
    tiles = list(tiles)
    step = 1
    while step < len(tiles):
        for i in range(len(tiles)):
            if i & step:
                continue
            u, v = tiles[i], tiles[i + step]
            tiles[i] = u - tan * v
            tiles[i + step] = v + tan * u
        step *= 2
    return tiles


def rotate_phase(re, im, half):
    c, s = cos_sin(half)
    return re * c + im * s, im * c - re * s


def sublane_mix(values, tan):
    place_in = lax.broadcasted_iota(jnp.int32, values.shape, 1)
    for step in (4, 2, 1):
        upper = (place_in // step) % 2 == 1
        below = pltpu.roll(values, step, 1)
        other = below if step == 4 else jnp.where(upper, below, pltpu.roll(values, 8 - step, 1))
        values = values + jnp.where(upper, tan, -tan) * other
    return values


def lane_table(cos, sin, scale):
    row = lax.broadcasted_iota(jnp.int32, (128, 128), 0)
    col = lax.broadcasted_iota(jnp.int32, (128, 128), 1)
    table = jnp.broadcast_to(scale, (128, 128))
    for bit in range(BITS):
        r = (row // 2**bit) % 2
        c = (col // 2**bit) % 2
        table = table * jnp.where(r == c, cos, jnp.where(r > c, -sin, sin))
    high = table.astype(jnp.bfloat16)
    low = (table - high.astype(jnp.float32)).astype(jnp.bfloat16)
    both = jnp.concatenate([high, low], axis=1)
    return jnp.concatenate([both, both], axis=0)


def lane_mix(values, table):
    high = values.astype(jnp.bfloat16)
    low = (values - high.astype(jnp.float32)).astype(jnp.bfloat16)
    parts = jnp.concatenate([high, low], axis=1)
    out = jnp.dot(parts, table, preferred_element_type=jnp.float32)
    return out[:, :128] + out[:, 128:]


def home_rows(src, dst, tan):
    def one(b, carry):
        tiles = butterfly([src[b * 8 + r] for r in range(8)], tan[0])
        for r in range(8):
            dst[b * 8 + r] = tiles[r]
        return carry

    lax.fori_loop(0, 16, one, 0, unroll=4)


def home_blocks(pick, pick_other, dst, r, tan):
    tiles = butterfly([pick(b * 8 + r) for b in range(16)], tan[1])
    for b in range(16):
        u, v = pick_other(b * 8 + r), tiles[b]
        dst[b, r, 0] = u - tan[0] * v
        dst[b, r, 1] = v + tan[0] * u


def finish(early, raw, tan, out, rows, stage, sems):
    copies = []
    for part in range(2):
        home_rows(raw.at[:, part], rows, tan)
        for r in range(8):
            home_blocks(lambda d: rows[d], lambda d: early[d, part], stage.at[part], r, tan)
            if r % 2:
                at = pl.ds(r - 1, 2)
                copies.append(
                    pltpu.make_async_copy(stage.at[part, :, at], out.at[part, :, at], sems.at[part, r // 2])
                )
                copies[-1].start()
    for copy in copies:
        copy.wait()


def kernel(amp, energy, diag_any, turn_any, early, raw, tan_out, diag, turn, a_in, e_in, e_rx, relay, fwd, mid, back, fin, tables, tans, sems, sends, recvs, met):
    bank, lane = place()
    me = bank * N_LANE + lane
    scope = jax.named_scope

    get_e = pltpu.make_async_copy(energy, e_in, sems.at[0])
    get_a = pltpu.make_async_copy(amp, a_in, sems.at[1])
    small = [pltpu.make_async_copy(diag_any, diag, sems.at[2]), pltpu.make_async_copy(turn_any, turn, sems.at[3])]
    for get in [get_e, *small]:
        get.start()

    spot = spots()
    devices = [spot(step) for step in STEPS]
    mixed = [spot(step) for step in MIXED]
    near = [spot(step)[0] for step in MIXED if lines(step) == 1]
    rounds = [pltpu.get_barrier_semaphore(), met.at[0], met.at[1]]

    def signal(n):
        for device in near:
            pl.semaphore_signal(rounds[n], 1, device_id=device, device_id_type=pl.DeviceIdType.MESH)

    def meet(n):
        with scope(f"meet_{n}"):
            pl.semaphore_wait(rounds[n], len(near))
        if n < 2:
            signal(n + 1)

    def send_e(n):
        some = [spot(step) for step in MIXED if lines(step) == n]
        send_all(some, lambda i: e_in.at[i], e_rx.at[me], sends.at[4], recvs.at[4])

    signal(0)
    with scope("wait_in"):
        get_e.wait()
    get_a.start()
    meet(0)
    with scope("send_e0"):
        send_e(1)
        for j, (step, line) in enumerate(RELAYED):
            device, _ = spot(along(step, line)[0])
            send(e_in.at[spot(step)[1]], relay.at[j], device, sends.at[4], recvs.at[5])
    e_rx[me] = e_in[me]

    with scope("tables"):
        for get in [*small, get_a]:
            get.wait()
        cos, sin = cos_sin(turn[...] * 0.5)
        tan = sin / cos
        for layer in range(2):
            for group in range(4):
                tans[layer, group] = jnp.broadcast_to(tan[layer : layer + 1, group : group + 1], (8, 128))
            c = [cos[layer : layer + 1, g : g + 1] for g in range(4)]
            c12 = c[1] * c[2]
            c12_2 = c12 * c12
            c3_2 = c[3] * c[3]
            scale = c12_2 * c12_2 * c12_2 * c12 * c3_2 * c3_2
            tables[layer] = lane_table(c[0], sin[layer : layer + 1, 0:1], scale)

    def first(i, carry):
        at = pl.ds(i * 8, 8)
        angle = (diag[0:1, :] * 0.5).reshape(1, 1, 1, 128)
        half = e_in[at] * angle
        re, im = rotate_phase(a_in[0, at], a_in[1, at], half)
        values = jnp.concatenate([re, im], axis=0)
        mixed = lane_mix(values.reshape(256, 128), tables[0]).reshape(32, 8, 128)
        mixed = sublane_mix(mixed, tans[0, 1, 0:1, :].reshape(1, 1, 128))
        mixed = mixed.reshape(2, 16, 8, 128)
        tan1 = tans[0, 1]
        for part in range(2):
            tiles = butterfly([mixed[part, j] for j in range(16)], tan1)
            for j in range(16):
                a_in[part, i * 8 + j // 2, j % 2] = tiles[j]
        return carry

    with scope("first_0"):
        lax.fori_loop(0, 4, first, 0, unroll=2)
    meet(1)
    send_e(2)
    with scope("first_1"):
        lax.fori_loop(4, 8, first, 0, unroll=2)
    with scope("wait_r"):
        wait_bytes(relay, recvs.at[5])
    with scope("relay"):
        for j, (step, line) in enumerate(RELAYED):
            part, rest = along(step, line)
            send(relay.at[j], e_rx.at[spot(reverse(part))[1]], spot(rest)[0], sends.at[5], recvs.at[4])
    with scope("first_2"):
        lax.fori_loop(8, 16, first, 0, unroll=2)
    meet(2)

    tan2 = tans[0, 2]
    for k in range(2):

        def blocks(i, carry):
            part, row = i // 8, lax.rem(i, 8)
            tiles = butterfly([a_in[part, b * 8 + row, k] for b in range(16)], tan2)
            for b in range(16):
                fwd[k, b * 8 + row, part] = tiles[b]
            return carry

        with scope(f"blocks_{k}"):
            lax.fori_loop(0, 16, blocks, 0, unroll=2)
        with scope(f"send_f{k}"):
            send_all(devices if k == 0 else mixed, lambda i: fwd.at[k, i], mid.at[k, me], sends.at[k], recvs.at[k])
        mid[k, me] = fwd[k, me]

    with scope("wait_e"):
        wait_bytes(e_rx.at[pl.ds(0, N_DEV - 1)], recvs.at[4])
    for k in range(2):
        with scope(f"wait_m{k}"):
            wait_bytes(mid.at[k, pl.ds(0, N_DEV - 1)], recvs.at[k])

        def lanes_1(i, carry):
            b, part = i // 2, lax.rem(i, 2)
            tiles = butterfly([mid[k, b * 16 + l, part] for l in range(16)], tans[0, 3])
            for l in range(16):
                mid[k, b * 16 + l, part] = tiles[l]
            return carry

        def banks(l, carry):
            re = butterfly([mid[k, b * 16 + l, 0] for b in range(8)], tans[0, 2])
            im = butterfly([mid[k, b * 16 + l, 1] for b in range(8)], tans[0, 2])
            angle = diag[1:2, :] * 0.5
            for b in range(8):
                re[b], im[b] = rotate_phase(re[b], im[b], e_rx[b * 16 + l, k] * angle)
            re = butterfly(re, tans[1, 2])
            im = butterfly(im, tans[1, 2])
            for b in range(8):
                mid[k, b * 16 + l, 0] = re[b]
                mid[k, b * 16 + l, 1] = im[b]
            return carry

        def lanes_2(b, carry):
            both = []
            for part in range(2):
                tiles = butterfly([mid[k, b * 16 + l, part] for l in range(16)], tans[1, 3])
                both.append(jnp.stack(tiles))
            values = jnp.stack(both).reshape(256, 128)
            mixed = lane_mix(values, tables[1]).reshape(32, 8, 128)
            mixed = sublane_mix(mixed, tans[1, 1, 0:1, :].reshape(1, 1, 128))
            mixed = mixed.reshape(2, 16, 8, 128)
            for part in range(2):
                back[k, pl.ds(b * 16, 16), part] = mixed[part]
            return carry

        with scope(f"mid_{k}"):
            lax.fori_loop(0, 16, lanes_1, 0, unroll=2)
            lax.fori_loop(0, 16, banks, 0, unroll=2)
            lax.fori_loop(0, 8, lanes_2, 0, unroll=2)
        home = fin if k == 0 else raw
        with scope(f"send_b{k}"):
            send_all(
                mixed if k == 0 else devices,
                lambda i: back.at[k, i],
                home.at[me],
                sends.at[2 + k],
                recvs.at[2 + k],
            )
        home[me] = back[k, me]

    with scope("wait_b0"):
        wait_bytes(fin.at[pl.ds(0, N_DEV - 1)], recvs.at[2])
    tan_out[0] = tans[1, 1]
    tan_out[1] = tans[1, 2]
    with scope("last_0"):
        for part in range(2):
            home_rows(fin.at[:, part], fin.at[:, part], tan_out)

            def last(r, carry):
                tiles = butterfly([fin[b * 8 + r, part] for b in range(16)], tan_out[1])
                for b in range(16):
                    early[b * 8 + r, part] = tiles[b]
                return carry

            lax.fori_loop(0, 8, last, 0, unroll=2)
    wait_bytes(e_in.at[pl.ds(0, N_DEV - 1)], sends.at[4])
    wait_bytes(relay, sends.at[5])
    for k in range(2):
        wait_bytes(fwd.at[k, pl.ds(0, N_DEV - 1)], sends.at[k])
        wait_bytes(back.at[k, pl.ds(0, N_DEV - 1)], sends.at[2 + k])
    with scope("wait_b1"):
        wait_bytes(raw.at[pl.ds(0, N_DEV - 1)], recvs.at[3])


def body(amplitudes, energies, diagonal_angles, turn_angles):
    f32 = jnp.float32
    anywhere = pl.BlockSpec(memory_space=pl.ANY)
    vmem = pl.BlockSpec(memory_space=pltpu.VMEM)
    early, raw, tan = pl.pallas_call(
        kernel,
        out_shape=(
            pltpu.VMEM((N_DEV, 2, 8, 128), f32),
            pltpu.VMEM((N_DEV, 2, 8, 128), f32),
            pltpu.VMEM((2, 8, 128), f32),
        ),
        in_specs=[anywhere] * 4,
        out_specs=(vmem,) * 3,
        scratch_shapes=[
            pltpu.VMEM((2, 128), f32),
            pltpu.VMEM((2, 4), f32),
            pltpu.VMEM((2, N_DEV, 2, 8, 128), f32),
            pltpu.VMEM((N_DEV, 2, 8, 128), f32),
            pltpu.VMEM((N_DEV, 2, 8, 128), f32),
            pltpu.VMEM((len(RELAYED), 2, 8, 128), f32),
            pltpu.VMEM((2, N_DEV, 2, 8, 128), f32),
            pltpu.VMEM((2, N_DEV, 2, 8, 128), f32),
            pltpu.VMEM((2, N_DEV, 2, 8, 128), f32),
            pltpu.VMEM((N_DEV, 2, 8, 128), f32),
            pltpu.VMEM((2, 256, 256), jnp.bfloat16),
            pltpu.VMEM((2, 4, 8, 128), f32),
            pltpu.SemaphoreType.DMA((4,)),
            pltpu.SemaphoreType.DMA((6,)),
            pltpu.SemaphoreType.DMA((6,)),
            pltpu.SemaphoreType.REGULAR((2,)),
        ],
        compiler_params=pltpu.CompilerParams(
            collective_id=0, has_side_effects=True, vmem_limit_bytes=24 * 1024 * 1024
        ),
        name="register",
    )(
        *(
            pltpu.with_memory_space_constraint(array, pltpu.HBM)
            for array in (
                amplitudes.reshape(2, N_DEV, 2, 8, 128),
                energies.reshape(N_DEV, 2, 8, 128),
                diagonal_angles,
                turn_angles,
            )
        )
    )
    out = pl.pallas_call(
        finish,
        out_shape=jax.ShapeDtypeStruct((2, 16, 8, 2, 8, 128), f32),
        in_specs=[vmem] * 3,
        out_specs=anywhere,
        scratch_shapes=[
            pltpu.VMEM((N_DEV, 8, 128), f32),
            pltpu.VMEM((2, 16, 8, 2, 8, 128), f32),
            pltpu.SemaphoreType.DMA((2, 4)),
        ],
        compiler_params=pltpu.CompilerParams(vmem_limit_bytes=8 * 1024 * 1024),
        name="finish",
    )(early, raw, tan)
    return out.reshape(2, 16, 128, 128)


def solution(mesh):
    split = P(None, ("bank", "lane"), None, None)
    in_specs = (split, P(("bank", "lane"), None, None), P(), P())
    return jax.shard_map(body, mesh=mesh, in_specs=in_specs, out_specs=split, check_vma=False)
```

```python
import itertools

import jax
import jax.numpy as jnp
from jax import lax
from jax.experimental import pallas as pl
from jax.experimental.pallas import tpu as pltpu
from jax.sharding import PartitionSpec as P

N_DEV = 128
N_LANE = 16
BITS = 7


def place():
    return lax.axis_index("bank"), lax.axis_index("lane")


def hops(step):
    return min(step, 4 - step)


STEPS = sorted(
    (s for s in itertools.product(range(4), range(2), range(4), range(4)) if any(s)),
    key=lambda s: -hops(s[0]) - hops(s[2]) - hops(s[3]),
)


MIXED = sorted(STEPS, key=lambda s: (s[0] * 11 + s[1] * 67 + s[2] * 83 + s[3] * 31) * 43 % 127)


def lines(step):
    return int(any(step[:2])) + int(step[2] > 0) + int(step[3] > 0)


def along(step, line):
    part = [(step[0], step[1], 0, 0), (0, 0, step[2], 0), (0, 0, 0, step[3])]
    rest = [(0, 0, step[2], step[3]), (step[0], step[1], 0, step[3]), (step[0], step[1], step[2], 0)]
    return part[line], rest[line]


def reverse(step):
    return ((4 - step[0]) % 4, step[1], (4 - step[2]) % 4, (4 - step[3]) % 4)


RELAYED = [(s, (s[0] * 2 + s[1] + s[2] + s[3]) % 3) for s in MIXED if lines(s) == 3]


def spots():
    bank, lane = place()
    x, core, z, y = bank // 2, lax.rem(bank, 2), lane // 4, lax.rem(lane, 4)
    xs = [lax.rem(x + s, 4) * 2 for s in range(4)]
    cores = [core, 1 - core]
    zs = [lax.rem(z + s, 4) * 4 for s in range(4)]
    ys = [lax.rem(y + s, 4) for s in range(4)]
    banks = {(i, j): xs[i] + cores[j] for i in range(4) for j in range(2)}
    lanes = {(i, j): zs[i] + ys[j] for i in range(4) for j in range(4)}

    def spot(step):
        to_bank, to_lane = banks[step[:2]], lanes[step[2:]]
        return (to_bank, to_lane), to_bank * N_LANE + to_lane

    return spot


def send(src, dst, device, send_sem, recv_sem):
    pltpu.make_async_remote_copy(
        src_ref=src,
        dst_ref=dst,
        send_sem=send_sem,
        recv_sem=recv_sem,
        device_id=device,
        device_id_type=pl.DeviceIdType.MESH,
    ).start()


def send_all(devices, pick_src, dst, send_sem, recv_sem):
    for device, index in devices:
        send(pick_src(index), dst, device, send_sem, recv_sem)


def wait_bytes(ref, sem):
    pltpu.make_async_copy(ref, ref, sem).wait()


def cos_sin(half):
    sq = half * half
    s = 1.0 / 6227020800.0
    for term in (-1.0 / 39916800.0, 1.0 / 362880.0, -1.0 / 5040.0, 1.0 / 120.0, -1.0 / 6.0):
        s = s * sq + term
    s = half + half * (sq * s)
    c = 1.0 / 479001600.0
    for term in (-1.0 / 3628800.0, 1.0 / 40320.0, -1.0 / 720.0, 1.0 / 24.0, -0.5):
        c = c * sq + term
    c = 1.0 + sq * c
    twice = s + s
    return 1.0 - twice * s, twice * c


def butterfly(tiles, tan):
    tiles = list(tiles)
    step = 1
    while step < len(tiles):
        for i in range(len(tiles)):
            if i & step:
                continue
            u, v = tiles[i], tiles[i + step]
            tiles[i] = u - tan * v
            tiles[i + step] = v + tan * u
        step *= 2
    return tiles


def rotate_phase(re, im, half):
    c, s = cos_sin(half)
    return re * c + im * s, im * c - re * s


def sublane_mix(values, tan):
    place_in = lax.broadcasted_iota(jnp.int32, values.shape, 1)
    for step in (4, 2, 1):
        upper = (place_in // step) % 2 == 1
        below = pltpu.roll(values, step, 1)
        other = below if step == 4 else jnp.where(upper, below, pltpu.roll(values, 8 - step, 1))
        values = values + jnp.where(upper, tan, -tan) * other
    return values


def lane_table(cos, sin, scale):
    row = lax.broadcasted_iota(jnp.int32, (128, 128), 0)
    col = lax.broadcasted_iota(jnp.int32, (128, 128), 1)
    table = jnp.broadcast_to(scale, (128, 128))
    for bit in range(BITS):
        r = (row // 2**bit) % 2
        c = (col // 2**bit) % 2
        table = table * jnp.where(r == c, cos, jnp.where(r > c, -sin, sin))
    high = table.astype(jnp.bfloat16)
    low = (table - high.astype(jnp.float32)).astype(jnp.bfloat16)
    both = jnp.concatenate([high, low], axis=1)
    return jnp.concatenate([both, both], axis=0)


def lane_mix(values, table):
    high = values.astype(jnp.bfloat16)
    low = (values - high.astype(jnp.float32)).astype(jnp.bfloat16)
    parts = jnp.concatenate([high, low], axis=1)
    out = jnp.dot(parts, table, preferred_element_type=jnp.float32)
    return out[:, :128] + out[:, 128:]


def home_rows(src, dst, tan):
    def one(b, carry):
        tiles = butterfly([src[b * 8 + r] for r in range(8)], tan[0])
        for r in range(8):
            dst[b * 8 + r] = tiles[r]
        return carry

    lax.fori_loop(0, 16, one, 0, unroll=4)


def home_blocks(pick, pick_other, dst, r, tan):
    tiles = butterfly([pick(b * 8 + r) for b in range(16)], tan[1])
    for b in range(16):
        u, v = pick_other(b * 8 + r), tiles[b]
        dst[b, r, 0] = u - tan[0] * v
        dst[b, r, 1] = v + tan[0] * u


def finish(early, raw, tan, out, rows, stage, sems):
    copies = []
    for part in range(2):
        home_rows(raw.at[:, part], rows, tan)
        for r in range(8):
            home_blocks(lambda d: rows[d], lambda d: early[d, part], stage.at[part], r, tan)
            if r % 2:
                at = pl.ds(r - 1, 2)
                copies.append(
                    pltpu.make_async_copy(stage.at[part, :, at], out.at[part, :, at], sems.at[part, r // 2])
                )
                copies[-1].start()
    for copy in copies:
        copy.wait()


def kernel(amp, energy, diag_any, turn_any, early, raw, tan_out, diag, turn, a_in, e_in, e_rx, relay, fwd, mid, back, fin, tables, tans, sems, sends, recvs, met):
    bank, lane = place()
    me = bank * N_LANE + lane
    scope = jax.named_scope

    get_e = pltpu.make_async_copy(energy, e_in, sems.at[0])
    get_a = pltpu.make_async_copy(amp, a_in, sems.at[1])
    small = [pltpu.make_async_copy(diag_any, diag, sems.at[2]), pltpu.make_async_copy(turn_any, turn, sems.at[3])]
    for get in [get_e, *small]:
        get.start()

    spot = spots()
    devices = [spot(step) for step in STEPS]
    mixed = [spot(step) for step in MIXED]
    near = [spot(step)[0] for step in MIXED if lines(step) == 1]
    rounds = [pltpu.get_barrier_semaphore(), met.at[0], met.at[1]]

    def signal(n):
        for device in near:
            pl.semaphore_signal(rounds[n], 1, device_id=device, device_id_type=pl.DeviceIdType.MESH)

    def meet(n):
        with scope(f"meet_{n}"):
            pl.semaphore_wait(rounds[n], len(near))
        if n < 2:
            signal(n + 1)

    def send_e(n):
        some = [spot(step) for step in MIXED if lines(step) == n]
        send_all(some, lambda i: e_in.at[i], e_rx.at[me], sends.at[4], recvs.at[4])

    signal(0)
    with scope("wait_in"):
        get_e.wait()
    get_a.start()
    meet(0)
    with scope("send_e0"):
        send_e(1)
        for j, (step, line) in enumerate(RELAYED):
            device, _ = spot(along(step, line)[0])
            send(e_in.at[spot(step)[1]], relay.at[j], device, sends.at[4], recvs.at[5])
    e_rx[me] = e_in[me]

    with scope("tables"):
        for get in [*small, get_a]:
            get.wait()
        cos, sin = cos_sin(turn[...] * 0.5)
        tan = sin / cos
        for layer in range(2):
            for group in range(4):
                tans[layer, group] = jnp.broadcast_to(tan[layer : layer + 1, group : group + 1], (8, 128))
            c = [cos[layer : layer + 1, g : g + 1] for g in range(4)]
            c12 = c[1] * c[2]
            c12_2 = c12 * c12
            c3_2 = c[3] * c[3]
            scale = c12_2 * c12_2 * c12_2 * c12 * c3_2 * c3_2
            tables[layer] = lane_table(c[0], sin[layer : layer + 1, 0:1], scale)

    def first(i, carry):
        at = pl.ds(i * 8, 8)
        angle = (diag[0:1, :] * 0.5).reshape(1, 1, 1, 128)
        half = e_in[at] * angle
        re, im = rotate_phase(a_in[0, at], a_in[1, at], half)
        values = jnp.concatenate([re, im], axis=0)
        mixed = lane_mix(values.reshape(256, 128), tables[0]).reshape(32, 8, 128)
        mixed = sublane_mix(mixed, tans[0, 1, 0:1, :].reshape(1, 1, 128))
        mixed = mixed.reshape(2, 16, 8, 128)
        tan1 = tans[0, 1]
        for part in range(2):
            tiles = butterfly([mixed[part, j] for j in range(16)], tan1)
            for j in range(16):
                a_in[part, i * 8 + j // 2, j % 2] = tiles[j]
        return carry

    with scope("first_0"):
        lax.fori_loop(0, 4, first, 0, unroll=2)
    meet(1)
    send_e(2)
    with scope("first_1"):
        lax.fori_loop(4, 8, first, 0, unroll=2)
    with scope("wait_r"):
        wait_bytes(relay, recvs.at[5])
    with scope("relay"):
        for j, (step, line) in enumerate(RELAYED):
            part, rest = along(step, line)
            send(relay.at[j], e_rx.at[spot(reverse(part))[1]], spot(rest)[0], sends.at[5], recvs.at[4])
    with scope("first_2"):
        lax.fori_loop(8, 16, first, 0, unroll=2)
    meet(2)

    tan2 = tans[0, 2]
    for k in range(2):

        def blocks(i, carry):
            part, row = i // 8, lax.rem(i, 8)
            tiles = butterfly([a_in[part, b * 8 + row, k] for b in range(16)], tan2)
            for b in range(16):
                fwd[k, b * 8 + row, part] = tiles[b]
            return carry

        with scope(f"blocks_{k}"):
            lax.fori_loop(0, 16, blocks, 0, unroll=2)
        with scope(f"send_f{k}"):
            send_all(devices if k == 0 else mixed, lambda i: fwd.at[k, i], mid.at[k, me], sends.at[k], recvs.at[k])
        mid[k, me] = fwd[k, me]

    with scope("wait_e"):
        wait_bytes(e_rx.at[pl.ds(0, N_DEV - 1)], recvs.at[4])
    for k in range(2):
        with scope(f"wait_m{k}"):
            wait_bytes(mid.at[k, pl.ds(0, N_DEV - 1)], recvs.at[k])

        def lanes_1(i, carry):
            b, part = i // 2, lax.rem(i, 2)
            tiles = butterfly([mid[k, b * 16 + l, part] for l in range(16)], tans[0, 3])
            for l in range(16):
                mid[k, b * 16 + l, part] = tiles[l]
            return carry

        def banks(l, carry):
            re = butterfly([mid[k, b * 16 + l, 0] for b in range(8)], tans[0, 2])
            im = butterfly([mid[k, b * 16 + l, 1] for b in range(8)], tans[0, 2])
            angle = diag[1:2, :] * 0.5
            for b in range(8):
                re[b], im[b] = rotate_phase(re[b], im[b], e_rx[b * 16 + l, k] * angle)
            re = butterfly(re, tans[1, 2])
            im = butterfly(im, tans[1, 2])
            for b in range(8):
                mid[k, b * 16 + l, 0] = re[b]
                mid[k, b * 16 + l, 1] = im[b]
            return carry

        def lanes_2(b, carry):
            both = []
            for part in range(2):
                tiles = butterfly([mid[k, b * 16 + l, part] for l in range(16)], tans[1, 3])
                both.append(jnp.stack(tiles))
            values = jnp.stack(both).reshape(256, 128)
            mixed = lane_mix(values, tables[1]).reshape(32, 8, 128)
            mixed = sublane_mix(mixed, tans[1, 1, 0:1, :].reshape(1, 1, 128))
            mixed = mixed.reshape(2, 16, 8, 128)
            for part in range(2):
                back[k, pl.ds(b * 16, 16), part] = mixed[part]
            return carry

        with scope(f"mid_{k}"):
            lax.fori_loop(0, 16, lanes_1, 0, unroll=2)
            lax.fori_loop(0, 16, banks, 0, unroll=2)
            lax.fori_loop(0, 8, lanes_2, 0, unroll=2)
        home = fin if k == 0 else raw
        with scope(f"send_b{k}"):
            send_all(
                mixed if k == 0 else devices,
                lambda i: back.at[k, i],
                home.at[me],
                sends.at[2 + k],
                recvs.at[2 + k],
            )
        home[me] = back[k, me]

    with scope("wait_b0"):
        wait_bytes(fin.at[pl.ds(0, N_DEV - 1)], recvs.at[2])
    tan_out[0] = tans[1, 1]
    tan_out[1] = tans[1, 2]
    with scope("last_0"):
        for part in range(2):
            home_rows(fin.at[:, part], fin.at[:, part], tan_out)

            def last(r, carry):
                tiles = butterfly([fin[b * 8 + r, part] for b in range(16)], tan_out[1])
                for b in range(16):
                    early[b * 8 + r, part] = tiles[b]
                return carry

            lax.fori_loop(0, 8, last, 0, unroll=2)
    wait_bytes(e_in.at[pl.ds(0, N_DEV - 1)], sends.at[4])
    wait_bytes(relay, sends.at[5])
    for k in range(2):
        wait_bytes(fwd.at[k, pl.ds(0, N_DEV - 1)], sends.at[k])
        wait_bytes(back.at[k, pl.ds(0, N_DEV - 1)], sends.at[2 + k])
    with scope("wait_b1"):
        wait_bytes(raw.at[pl.ds(0, N_DEV - 1)], recvs.at[3])


def body(amplitudes, energies, diagonal_angles, turn_angles):
    f32 = jnp.float32
    anywhere = pl.BlockSpec(memory_space=pl.ANY)
    vmem = pl.BlockSpec(memory_space=pltpu.VMEM)
    early, raw, tan = pl.pallas_call(
        kernel,
        out_shape=(
            pltpu.VMEM((N_DEV, 2, 8, 128), f32),
            pltpu.VMEM((N_DEV, 2, 8, 128), f32),
            pltpu.VMEM((2, 8, 128), f32),
        ),
        in_specs=[anywhere] * 4,
        out_specs=(vmem,) * 3,
        scratch_shapes=[
            pltpu.VMEM((2, 128), f32),
            pltpu.VMEM((2, 4), f32),
            pltpu.VMEM((2, N_DEV, 2, 8, 128), f32),
            pltpu.VMEM((N_DEV, 2, 8, 128), f32),
            pltpu.VMEM((N_DEV, 2, 8, 128), f32),
            pltpu.VMEM((len(RELAYED), 2, 8, 128), f32),
            pltpu.VMEM((2, N_DEV, 2, 8, 128), f32),
            pltpu.VMEM((2, N_DEV, 2, 8, 128), f32),
            pltpu.VMEM((2, N_DEV, 2, 8, 128), f32),
            pltpu.VMEM((N_DEV, 2, 8, 128), f32),
            pltpu.VMEM((2, 256, 256), jnp.bfloat16),
            pltpu.VMEM((2, 4, 8, 128), f32),
            pltpu.SemaphoreType.DMA((4,)),
            pltpu.SemaphoreType.DMA((6,)),
            pltpu.SemaphoreType.DMA((6,)),
            pltpu.SemaphoreType.REGULAR((2,)),
        ],
        compiler_params=pltpu.CompilerParams(
            collective_id=0, has_side_effects=True, vmem_limit_bytes=24 * 1024 * 1024
        ),
        name="register",
    )(
        *(
            pltpu.with_memory_space_constraint(array, pltpu.HBM)
            for array in (
                amplitudes.reshape(2, N_DEV, 2, 8, 128),
                energies.reshape(N_DEV, 2, 8, 128),
                diagonal_angles,
                turn_angles,
            )
        )
    )
    out = pl.pallas_call(
        finish,
        out_shape=jax.ShapeDtypeStruct((2, 16, 8, 2, 8, 128), f32),
        in_specs=[vmem] * 3,
        out_specs=anywhere,
        scratch_shapes=[
            pltpu.VMEM((N_DEV, 8, 128), f32),
            pltpu.VMEM((2, 16, 8, 2, 8, 128), f32),
            pltpu.SemaphoreType.DMA((2, 4)),
        ],
        compiler_params=pltpu.CompilerParams(vmem_limit_bytes=8 * 1024 * 1024),
        name="finish",
    )(early, raw, tan)
    return out.reshape(2, 16, 128, 128)


def solution(mesh):
    split = P(None, ("bank", "lane"), None, None)
    in_specs = (split, P(("bank", "lane"), None, None), P(), P())
    return jax.shard_map(body, mesh=mesh, in_specs=in_specs, out_specs=split, check_vma=False)
```

```python
import itertools

import jax
import jax.numpy as jnp
from jax import lax
from jax.experimental import pallas as pl
from jax.experimental.pallas import tpu as pltpu
from jax.sharding import PartitionSpec as P

N_DEV = 128
N_LANE = 16
BITS = 7


def place():
    return lax.axis_index("bank"), lax.axis_index("lane")


def hops(step):
    return min(step, 4 - step)


STEPS = sorted(
    (s for s in itertools.product(range(4), range(2), range(4), range(4)) if any(s)),
    key=lambda s: -hops(s[0]) - hops(s[2]) - hops(s[3]),
)


MIXED = sorted(STEPS, key=lambda s: (s[0] * 11 + s[1] * 67 + s[2] * 83 + s[3] * 31) * 43 % 127)


def lines(step):
    return int(any(step[:2])) + int(step[2] > 0) + int(step[3] > 0)


def along(step, line):
    part = [(step[0], step[1], 0, 0), (0, 0, step[2], 0), (0, 0, 0, step[3])]
    rest = [(0, 0, step[2], step[3]), (step[0], step[1], 0, step[3]), (step[0], step[1], step[2], 0)]
    return part[line], rest[line]


def reverse(step):
    return ((4 - step[0]) % 4, step[1], (4 - step[2]) % 4, (4 - step[3]) % 4)


RELAYED = [(s, (s[0] * 2 + s[1] + s[2] + s[3]) % 3) for s in MIXED if lines(s) == 3]


def spots():
    bank, lane = place()
    x, core, z, y = bank // 2, lax.rem(bank, 2), lane // 4, lax.rem(lane, 4)
    xs = [lax.rem(x + s, 4) * 2 for s in range(4)]
    cores = [core, 1 - core]
    zs = [lax.rem(z + s, 4) * 4 for s in range(4)]
    ys = [lax.rem(y + s, 4) for s in range(4)]
    banks = {(i, j): xs[i] + cores[j] for i in range(4) for j in range(2)}
    lanes = {(i, j): zs[i] + ys[j] for i in range(4) for j in range(4)}

    def spot(step):
        to_bank, to_lane = banks[step[:2]], lanes[step[2:]]
        return (to_bank, to_lane), to_bank * N_LANE + to_lane

    return spot


def send(src, dst, device, send_sem, recv_sem):
    pltpu.make_async_remote_copy(
        src_ref=src,
        dst_ref=dst,
        send_sem=send_sem,
        recv_sem=recv_sem,
        device_id=device,
        device_id_type=pl.DeviceIdType.MESH,
    ).start()


def send_all(devices, pick_src, dst, send_sem, recv_sem):
    for device, index in devices:
        send(pick_src(index), dst, device, send_sem, recv_sem)


def wait_bytes(ref, sem):
    pltpu.make_async_copy(ref, ref, sem).wait()


def cos_sin(half):
    sq = half * half
    s = 1.0 / 6227020800.0
    for term in (-1.0 / 39916800.0, 1.0 / 362880.0, -1.0 / 5040.0, 1.0 / 120.0, -1.0 / 6.0):
        s = s * sq + term
    s = half + half * (sq * s)
    c = 1.0 / 479001600.0
    for term in (-1.0 / 3628800.0, 1.0 / 40320.0, -1.0 / 720.0, 1.0 / 24.0, -0.5):
        c = c * sq + term
    c = 1.0 + sq * c
    twice = s + s
    return 1.0 - twice * s, twice * c


def butterfly(tiles, tan):
    tiles = list(tiles)
    step = 1
    while step < len(tiles):
        for i in range(len(tiles)):
            if i & step:
                continue
            u, v = tiles[i], tiles[i + step]
            tiles[i] = u - tan * v
            tiles[i + step] = v + tan * u
        step *= 2
    return tiles


def rotate_phase(re, im, half):
    c, s = cos_sin(half)
    return re * c + im * s, im * c - re * s


def sublane_mix(values, tan):
    place_in = lax.broadcasted_iota(jnp.int32, values.shape, 1)
    for step in (4, 2, 1):
        upper = (place_in // step) % 2 == 1
        below = pltpu.roll(values, step, 1)
        other = below if step == 4 else jnp.where(upper, below, pltpu.roll(values, 8 - step, 1))
        values = values + jnp.where(upper, tan, -tan) * other
    return values


def lane_table(cos, sin, scale):
    row = lax.broadcasted_iota(jnp.int32, (128, 128), 0)
    col = lax.broadcasted_iota(jnp.int32, (128, 128), 1)
    table = jnp.broadcast_to(scale, (128, 128))
    for bit in range(BITS):
        r = (row // 2**bit) % 2
        c = (col // 2**bit) % 2
        table = table * jnp.where(r == c, cos, jnp.where(r > c, -sin, sin))
    high = table.astype(jnp.bfloat16)
    low = (table - high.astype(jnp.float32)).astype(jnp.bfloat16)
    both = jnp.concatenate([high, low], axis=1)
    return jnp.concatenate([both, both], axis=0)


def lane_mix(values, table):
    high = values.astype(jnp.bfloat16)
    low = (values - high.astype(jnp.float32)).astype(jnp.bfloat16)
    parts = jnp.concatenate([high, low], axis=1)
    out = jnp.dot(parts, table, preferred_element_type=jnp.float32)
    return out[:, :128] + out[:, 128:]


def home_rows(src, dst, tan):
    def one(b, carry):
        tiles = butterfly([src[b * 8 + r] for r in range(8)], tan[0])
        for r in range(8):
            dst[b * 8 + r] = tiles[r]
        return carry

    lax.fori_loop(0, 16, one, 0, unroll=4)


def home_blocks(pick, pick_other, dst, r, tan):
    tiles = butterfly([pick(b * 8 + r) for b in range(16)], tan[1])
    for b in range(16):
        u, v = pick_other(b * 8 + r), tiles[b]
        dst[b, r, 0] = u - tan[0] * v
        dst[b, r, 1] = v + tan[0] * u


def finish(early, raw, tan, out, rows, stage, sems):
    copies = []
    for part in range(2):
        home_rows(raw.at[:, part], rows, tan)
        for r in range(8):
            home_blocks(lambda d: rows[d], lambda d: early[d, part], stage.at[part], r, tan)
            if r % 2:
                at = pl.ds(r - 1, 2)
                copies.append(
                    pltpu.make_async_copy(stage.at[part, :, at], out.at[part, :, at], sems.at[part, r // 2])
                )
                copies[-1].start()
    for copy in copies:
        copy.wait()


def kernel(amp, energy, diag_any, turn_any, early, raw, tan_out, diag, turn, a_in, e_in, e_rx, relay, fwd, mid, back, fin, tables, tans, sems, sends, recvs, met):
    bank, lane = place()
    me = bank * N_LANE + lane
    scope = jax.named_scope

    get_e = pltpu.make_async_copy(energy, e_in, sems.at[0])
    get_a = pltpu.make_async_copy(amp, a_in, sems.at[1])
    small = [pltpu.make_async_copy(diag_any, diag, sems.at[2]), pltpu.make_async_copy(turn_any, turn, sems.at[3])]
    for get in [get_e, *small]:
        get.start()

    spot = spots()
    devices = [spot(step) for step in STEPS]
    mixed = [spot(step) for step in MIXED]
    near = [spot(step)[0] for step in MIXED if lines(step) == 1]
    rounds = [pltpu.get_barrier_semaphore(), met.at[0], met.at[1]]

    def signal(n):
        for device in near:
            pl.semaphore_signal(rounds[n], 1, device_id=device, device_id_type=pl.DeviceIdType.MESH)

    def meet(n):
        with scope(f"meet_{n}"):
            pl.semaphore_wait(rounds[n], len(near))
        if n < 2:
            signal(n + 1)

    def send_e(n):
        some = [spot(step) for step in MIXED if lines(step) == n]
        send_all(some, lambda i: e_in.at[i], e_rx.at[me], sends.at[4], recvs.at[4])

    signal(0)
    with scope("wait_in"):
        get_e.wait()
    get_a.start()
    meet(0)
    with scope("send_e0"):
        send_e(1)
        for j, (step, line) in enumerate(RELAYED):
            device, _ = spot(along(step, line)[0])
            send(e_in.at[spot(step)[1]], relay.at[j], device, sends.at[4], recvs.at[5])
    e_rx[me] = e_in[me]

    with scope("tables"):
        for get in [*small, get_a]:
            get.wait()
        cos, sin = cos_sin(turn[...] * 0.5)
        tan = sin / cos
        for layer in range(2):
            for group in range(4):
                tans[layer, group] = jnp.broadcast_to(tan[layer : layer + 1, group : group + 1], (8, 128))
            c = [cos[layer : layer + 1, g : g + 1] for g in range(4)]
            c12 = c[1] * c[2]
            c12_2 = c12 * c12
            c3_2 = c[3] * c[3]
            scale = c12_2 * c12_2 * c12_2 * c12 * c3_2 * c3_2
            tables[layer] = lane_table(c[0], sin[layer : layer + 1, 0:1], scale)

    def first(i, carry):
        at = pl.ds(i * 8, 8)
        angle = (diag[0:1, :] * 0.5).reshape(1, 1, 1, 128)
        half = e_in[at] * angle
        re, im = rotate_phase(a_in[0, at], a_in[1, at], half)
        values = jnp.concatenate([re, im], axis=0)
        mixed = lane_mix(values.reshape(256, 128), tables[0]).reshape(32, 8, 128)
        mixed = sublane_mix(mixed, tans[0, 1, 0:1, :].reshape(1, 1, 128))
        mixed = mixed.reshape(2, 16, 8, 128)
        tan1 = tans[0, 1]
        for part in range(2):
            tiles = butterfly([mixed[part, j] for j in range(16)], tan1)
            for j in range(16):
                a_in[part, i * 8 + j // 2, j % 2] = tiles[j]
        return carry

    with scope("first_0"):
        lax.fori_loop(0, 4, first, 0, unroll=2)
    meet(1)
    send_e(2)
    with scope("first_1"):
        lax.fori_loop(4, 8, first, 0, unroll=2)
    with scope("wait_r"):
        wait_bytes(relay, recvs.at[5])
    with scope("relay"):
        for j, (step, line) in enumerate(RELAYED):
            part, rest = along(step, line)
            send(relay.at[j], e_rx.at[spot(reverse(part))[1]], spot(rest)[0], sends.at[5], recvs.at[4])
    with scope("first_2"):
        lax.fori_loop(8, 16, first, 0, unroll=2)
    meet(2)

    tan2 = tans[0, 2]
    for k in range(2):

        def blocks(i, carry):
            part, row = i // 8, lax.rem(i, 8)
            tiles = butterfly([a_in[part, b * 8 + row, k] for b in range(16)], tan2)
            for b in range(16):
                fwd[k, b * 8 + row, part] = tiles[b]
            return carry

        with scope(f"blocks_{k}"):
            lax.fori_loop(0, 16, blocks, 0, unroll=2)
        with scope(f"send_f{k}"):
            send_all(devices if k == 0 else mixed, lambda i: fwd.at[k, i], mid.at[k, me], sends.at[k], recvs.at[k])
        mid[k, me] = fwd[k, me]

    with scope("wait_e"):
        wait_bytes(e_rx.at[pl.ds(0, N_DEV - 1)], recvs.at[4])
    for k in range(2):
        with scope(f"wait_m{k}"):
            wait_bytes(mid.at[k, pl.ds(0, N_DEV - 1)], recvs.at[k])

        def lanes_1(i, carry):
            b, part = i // 2, lax.rem(i, 2)
            tiles = butterfly([mid[k, b * 16 + l, part] for l in range(16)], tans[0, 3])
            for l in range(16):
                mid[k, b * 16 + l, part] = tiles[l]
            return carry

        def banks(l, carry):
            re = butterfly([mid[k, b * 16 + l, 0] for b in range(8)], tans[0, 2])
            im = butterfly([mid[k, b * 16 + l, 1] for b in range(8)], tans[0, 2])
            angle = diag[1:2, :] * 0.5
            for b in range(8):
                re[b], im[b] = rotate_phase(re[b], im[b], e_rx[b * 16 + l, k] * angle)
            re = butterfly(re, tans[1, 2])
            im = butterfly(im, tans[1, 2])
            for b in range(8):
                mid[k, b * 16 + l, 0] = re[b]
                mid[k, b * 16 + l, 1] = im[b]
            return carry

        def lanes_2(b, carry):
            both = []
            for part in range(2):
                tiles = butterfly([mid[k, b * 16 + l, part] for l in range(16)], tans[1, 3])
                both.append(jnp.stack(tiles))
            values = jnp.stack(both).reshape(256, 128)
            mixed = lane_mix(values, tables[1]).reshape(32, 8, 128)
            mixed = sublane_mix(mixed, tans[1, 1, 0:1, :].reshape(1, 1, 128))
            mixed = mixed.reshape(2, 16, 8, 128)
            for part in range(2):
                back[k, pl.ds(b * 16, 16), part] = mixed[part]
            return carry

        with scope(f"mid_{k}"):
            lax.fori_loop(0, 16, lanes_1, 0, unroll=4)
            lax.fori_loop(0, 16, banks, 0, unroll=4)
            lax.fori_loop(0, 8, lanes_2, 0, unroll=4)
        home = fin if k == 0 else raw
        with scope(f"send_b{k}"):
            send_all(
                mixed if k == 0 else devices,
                lambda i: back.at[k, i],
                home.at[me],
                sends.at[2 + k],
                recvs.at[2 + k],
            )
        home[me] = back[k, me]

    with scope("wait_b0"):
        wait_bytes(fin.at[pl.ds(0, N_DEV - 1)], recvs.at[2])
    tan_out[0] = tans[1, 1]
    tan_out[1] = tans[1, 2]
    with scope("last_0"):
        for part in range(2):
            home_rows(fin.at[:, part], fin.at[:, part], tan_out)

            def last(r, carry):
                tiles = butterfly([fin[b * 8 + r, part] for b in range(16)], tan_out[1])
                for b in range(16):
                    early[b * 8 + r, part] = tiles[b]
                return carry

            lax.fori_loop(0, 8, last, 0, unroll=2)
    wait_bytes(e_in.at[pl.ds(0, N_DEV - 1)], sends.at[4])
    wait_bytes(relay, sends.at[5])
    for k in range(2):
        wait_bytes(fwd.at[k, pl.ds(0, N_DEV - 1)], sends.at[k])
        wait_bytes(back.at[k, pl.ds(0, N_DEV - 1)], sends.at[2 + k])
    with scope("wait_b1"):
        wait_bytes(raw.at[pl.ds(0, N_DEV - 1)], recvs.at[3])


def body(amplitudes, energies, diagonal_angles, turn_angles):
    f32 = jnp.float32
    anywhere = pl.BlockSpec(memory_space=pl.ANY)
    vmem = pl.BlockSpec(memory_space=pltpu.VMEM)
    early, raw, tan = pl.pallas_call(
        kernel,
        out_shape=(
            pltpu.VMEM((N_DEV, 2, 8, 128), f32),
            pltpu.VMEM((N_DEV, 2, 8, 128), f32),
            pltpu.VMEM((2, 8, 128), f32),
        ),
        in_specs=[anywhere] * 4,
        out_specs=(vmem,) * 3,
        scratch_shapes=[
            pltpu.VMEM((2, 128), f32),
            pltpu.VMEM((2, 4), f32),
            pltpu.VMEM((2, N_DEV, 2, 8, 128), f32),
            pltpu.VMEM((N_DEV, 2, 8, 128), f32),
            pltpu.VMEM((N_DEV, 2, 8, 128), f32),
            pltpu.VMEM((len(RELAYED), 2, 8, 128), f32),
            pltpu.VMEM((2, N_DEV, 2, 8, 128), f32),
            pltpu.VMEM((2, N_DEV, 2, 8, 128), f32),
            pltpu.VMEM((2, N_DEV, 2, 8, 128), f32),
            pltpu.VMEM((N_DEV, 2, 8, 128), f32),
            pltpu.VMEM((2, 256, 256), jnp.bfloat16),
            pltpu.VMEM((2, 4, 8, 128), f32),
            pltpu.SemaphoreType.DMA((4,)),
            pltpu.SemaphoreType.DMA((6,)),
            pltpu.SemaphoreType.DMA((6,)),
            pltpu.SemaphoreType.REGULAR((2,)),
        ],
        compiler_params=pltpu.CompilerParams(
            collective_id=0, has_side_effects=True, vmem_limit_bytes=24 * 1024 * 1024
        ),
        name="register",
    )(
        *(
            pltpu.with_memory_space_constraint(array, pltpu.HBM)
            for array in (
                amplitudes.reshape(2, N_DEV, 2, 8, 128),
                energies.reshape(N_DEV, 2, 8, 128),
                diagonal_angles,
                turn_angles,
            )
        )
    )
    out = pl.pallas_call(
        finish,
        out_shape=jax.ShapeDtypeStruct((2, 16, 8, 2, 8, 128), f32),
        in_specs=[vmem] * 3,
        out_specs=anywhere,
        scratch_shapes=[
            pltpu.VMEM((N_DEV, 8, 128), f32),
            pltpu.VMEM((2, 16, 8, 2, 8, 128), f32),
            pltpu.SemaphoreType.DMA((2, 4)),
        ],
        compiler_params=pltpu.CompilerParams(vmem_limit_bytes=8 * 1024 * 1024),
        name="finish",
    )(early, raw, tan)
    return out.reshape(2, 16, 128, 128)


def solution(mesh):
    split = P(None, ("bank", "lane"), None, None)
    in_specs = (split, P(("bank", "lane"), None, None), P(), P())
    return jax.shard_map(body, mesh=mesh, in_specs=in_specs, out_specs=split, check_vma=False)
```
